8 devices in a mesh: dp: 1 (over z), tp: 8 (over y, x, core).
Axes of the slice: x: 2, y: 2, z: 1, core: 2. Of those that a mesh axis runs over, the one named last changes fastest.
Arguments:
- hidden: bfloat16 [3, 4096], P('dp')
- positions: int32 [3], P('dp')
- k_local: bfloat16 [3, 4096, 8, 128], P('dp', None, 'tp')
- v_local: bfloat16 [3, 4096, 8, 128], P('dp', None, 'tp')
- k_global: bfloat16 [3, 24576, 8, 128], P('dp', None, 'tp')
- v_global: bfloat16 [3, 24576, 8, 128], P('dp', None, 'tp')
- w_query: bfloat16 [2, 4096, 4096], P(None, None, 'tp')
- w_key: bfloat16 [2, 4096, 1024], P(None, None, 'tp')
- w_value: bfloat16 [2, 4096, 1024], P(None, None, 'tp')
- w_out: bfloat16 [2, 4096, 4096], P(None, 'tp')
- w_gate: bfloat16 [2, 4096, 14336], P(None, None, 'tp')
- w_up: bfloat16 [2, 4096, 14336], P(None, None, 'tp')
- w_down: bfloat16 [2, 14336, 4096], P(None, 'tp')
- norm_scale: float32 [2, 4, 4096], replicated
Outputs:
- output 1: bfloat16 [3, 4096], P('dp')
- output 2: bfloat16 [3, 4096, 8, 128], P('dp', None, 'tp')
- output 3: bfloat16 [3, 4096, 8, 128], P('dp', None, 'tp')
- output 4: bfloat16 [3, 24576, 8, 128], P('dp', None, 'tp')
- output 5: bfloat16 [3, 24576, 8, 128], P('dp', None, 'tp')
All inputs are finite; a program needn't handle non-finite values.
Results may differ from the reference program's by a relative error of at most 0.02.
Values are sent between devices in bfloat16 or wider.
A program may use at most 1 GiB of HBM per device.

```python
import jax
import jax.numpy as jnp
from jax import lax

D = 4096
HEADS = 32
KV_HEADS = 8
HEAD = 128
FF = 14336
WINDOW = 4096
BATCH = 3
CTX = 24576

SOFT_CAP = 50.0
NORM_EPS = 1e-6
ROPE_BASE = 10000.0
NEG_FILL = -1e30


def draw_positions(pos_key):
    draw_key, row_key = jax.random.split(pos_key)
    drawn_pos = jax.random.randint(draw_key, (BATCH,), WINDOW, CTX, dtype=jnp.int32)
    top_row = jax.random.randint(row_key, (), 0, BATCH, dtype=jnp.int32)
    row_ids = jnp.arange(BATCH, dtype=jnp.int32)
    return jnp.where(row_ids == top_row, CTX - 1, drawn_pos).astype(jnp.int32)


def normal_bf16(rand_key, arr_shape, std_scale):
    return (jax.random.normal(rand_key, arr_shape, jnp.float32) * std_scale).astype(jnp.bfloat16)


def setup_inputs(seed: int = 0, part: int = 0) -> dict:
    part_key = jax.random.fold_in(jax.random.key(seed), part)
    row_keys = jax.random.split(part_key, 6)
    weight_keys = jax.random.split(jax.random.key(seed + 1), 8)
    value_gain = jnp.sqrt(jnp.array([WINDOW, CTX], dtype=jnp.float32)).reshape(2, 1, 1)
    return {
        'hidden': normal_bf16(row_keys[0], (BATCH, D), 1.0),
        'positions': draw_positions(row_keys[1]),
        'k_local': normal_bf16(row_keys[2], (BATCH, WINDOW, KV_HEADS, HEAD), 1.0),
        'v_local': normal_bf16(row_keys[3], (BATCH, WINDOW, KV_HEADS, HEAD), 1.0),
        'k_global': normal_bf16(row_keys[4], (BATCH, CTX, KV_HEADS, HEAD), 1.0),
        'v_global': normal_bf16(row_keys[5], (BATCH, CTX, KV_HEADS, HEAD), 1.0),
        'w_query': normal_bf16(weight_keys[0], (2, D, HEADS * HEAD), D ** -0.5),
        'w_key': normal_bf16(weight_keys[1], (2, D, KV_HEADS * HEAD), D ** -0.5),
        'w_value': normal_bf16(weight_keys[2], (2, D, KV_HEADS * HEAD), value_gain * D ** -0.5),
        'w_out': normal_bf16(weight_keys[3], (2, HEADS * HEAD, D), (HEADS * HEAD) ** -0.5),
        'w_gate': normal_bf16(weight_keys[4], (2, D, FF), D ** -0.5),
        'w_up': normal_bf16(weight_keys[5], (2, D, FF), D ** -0.5),
        'w_down': normal_bf16(weight_keys[6], (2, FF, D), FF ** -0.5),
        'norm_scale': jax.random.normal(weight_keys[7], (2, 4, D), jnp.float32) * 0.4,
    }


def rms_norm(values, gain_row):
    values_f32 = values.astype(jnp.float32)
    inv_rms = lax.rsqrt(jnp.mean(values_f32 * values_f32, axis=-1, keepdims=True) + NORM_EPS)
    return (values_f32 * inv_rms * (1.0 + gain_row)).astype(jnp.bfloat16)


def rotary(projected, positions):
    half_dim = HEAD // 2
    inv_freq = ROPE_BASE ** (-2.0 * jnp.arange(half_dim, dtype=jnp.float32) / HEAD)
    angles = positions.astype(jnp.float32)[:, None, None] * inv_freq
    cos_part = jnp.cos(angles)
    sin_part = jnp.sin(angles)
    first_half = projected[..., :half_dim]
    second_half = projected[..., half_dim:]
    return jnp.concatenate([first_half * cos_part - second_half * sin_part, second_half * cos_part + first_half * sin_part], axis=-1)


def attend_row(row_args):
    queries, key_rows, value_rows, key_valid = row_args
    logits = jnp.einsum('grd,ngd->grn', queries.astype(jnp.float32), key_rows.astype(jnp.float32)) * HEAD ** -0.5
    logits = SOFT_CAP * jnp.tanh(logits / SOFT_CAP)
    logits = jnp.where(key_valid[None, None, :], logits, NEG_FILL)
    attn_probs = jax.nn.softmax(logits, axis=-1).astype(jnp.bfloat16)
    mixed_heads = jnp.einsum('grn,ngd->grd', attn_probs.astype(jnp.float32), value_rows.astype(jnp.float32))
    return mixed_heads.astype(jnp.bfloat16)


def add_normed(hidden, branch_sum, gain_row):
    return (hidden.astype(jnp.float32) + rms_norm(branch_sum, gain_row).astype(jnp.float32)).astype(jnp.bfloat16)


def decoder_layer(hidden, positions, k_cache, v_cache, slot_ids, key_valid, layer_weights, gains):
    w_query, w_key, w_value, w_out, w_gate, w_up, w_down = layer_weights
    normed = rms_norm(hidden, gains[0])
    queries = jnp.dot(normed, w_query, preferred_element_type=jnp.float32).reshape(BATCH, HEADS, HEAD)
    key_new = jnp.dot(normed, w_key, preferred_element_type=jnp.float32).reshape(BATCH, KV_HEADS, HEAD)
    value_new = jnp.dot(normed, w_value, preferred_element_type=jnp.float32).astype(jnp.bfloat16).reshape(BATCH, KV_HEADS, HEAD)
    queries = rotary(queries, positions).astype(jnp.bfloat16)
    key_new = rotary(key_new, positions).astype(jnp.bfloat16)
    slot_hit = (jnp.arange(k_cache.shape[1])[None, :] == slot_ids[:, None])[:, :, None, None]
    k_cache = jnp.where(slot_hit, key_new[:, None], k_cache)
    v_cache = jnp.where(slot_hit, value_new[:, None], v_cache)
    grouped = queries.reshape(BATCH, KV_HEADS, HEADS // KV_HEADS, HEAD)
    mixed_heads = lax.map(attend_row, (grouped, k_cache, v_cache, key_valid))
    attn_sum = jnp.dot(mixed_heads.reshape(BATCH, HEADS * HEAD), w_out, preferred_element_type=jnp.float32)
    hidden = add_normed(hidden, attn_sum, gains[1])
    normed = rms_norm(hidden, gains[2])
    gate_proj = jnp.dot(normed, w_gate, preferred_element_type=jnp.float32)
    up_proj = jnp.dot(normed, w_up, preferred_element_type=jnp.float32)
    hidden_act = (jax.nn.gelu(gate_proj, approximate=True) * up_proj).astype(jnp.bfloat16)
    down_sum = jnp.dot(hidden_act, w_down, preferred_element_type=jnp.float32)
    hidden = add_normed(hidden, down_sum, gains[3])
    return hidden, k_cache, v_cache


def reference(hidden, positions, k_local, v_local, k_global, v_global, w_query, w_key, w_value, w_out, w_gate, w_up, w_down, norm_scale):
    stacks = (w_query, w_key, w_value, w_out, w_gate, w_up, w_down)
    local_valid = jnp.full((BATCH, WINDOW), True)
    global_valid = jnp.arange(CTX)[None, :] <= positions[:, None]
    hidden, k_local, v_local = decoder_layer(hidden, positions, k_local, v_local, positions % WINDOW, local_valid, tuple(stacked[0] for stacked in stacks), norm_scale[0])
    hidden, k_global, v_global = decoder_layer(hidden, positions, k_global, v_global, positions, global_valid, tuple(stacked[1] for stacked in stacks), norm_scale[1])
    return (hidden, k_local, v_local, k_global, v_global)
```

```python
import functools

import jax
import jax.numpy as jnp
import numpy as np
from jax import lax
from jax.experimental import pallas as pl
from jax.experimental.pallas import tpu as pltpu
from jax.sharding import PartitionSpec as P

SOFT_CAP = 50.0
NORM_EPS = 1e-6
ROPE_BASE = 10000.0
HEAD = 128
MIB = 1024 * 1024
F32 = jnp.float32
BF16 = jnp.bfloat16


def norm_rows(values, gain_row):
    inv_rms = lax.rsqrt(jnp.mean(values * values, axis=-1, keepdims=True) + NORM_EPS)
    return (values * inv_rms * (1.0 + gain_row)).astype(BF16)


def matmul(lhs, rhs):
    return jnp.dot(lhs, rhs, preferred_element_type=F32)


def rotate(head, cos_part, sin_part):
    return head * cos_part + pltpu.roll(head, HEAD // 2, 1) * sin_part


def attn_kernel(layer, block, ahead, window, pos_ref, freq_ref, x_ref, gain_ref, wq_hbm, wk_hbm, wv_hbm, wo_hbm, k_hbm, v_hbm,
                o_ref, k_out, v_out, kbuf, vbuf, wq, wk, wv, wo, xbuf, ebuf, w_sem, kin_sem, vin_sem, kout_sem, vout_sem):
    batch, length = k_hbm.shape[0], k_hbm.shape[1]
    heads = wq.shape[1] // HEAD
    blocks = length // block

    def k_in(i):
        rows = pl.ds(i * block, block)
        return pltpu.make_async_copy(k_hbm.at[:, rows, :], kbuf.at[:, rows, :], kin_sem.at[i])

    def v_in(i):
        rows = pl.ds(i * block, block)
        return pltpu.make_async_copy(v_hbm.at[:, rows, :], vbuf.at[:, rows, :], vin_sem.at[i])

    def k_back(i):
        rows = pl.ds(i * block, block)
        return pltpu.make_async_copy(kbuf.at[:, rows, :], k_out.at[:, rows, :], kout_sem.at[i])

    def v_back(i):
        rows = pl.ds(i * block, block)
        return pltpu.make_async_copy(vbuf.at[:, rows, :], v_out.at[:, rows, :], vout_sem.at[i])

    wq_copy = pltpu.make_async_copy(wq_hbm.at[layer], wq, w_sem.at[0])
    wk_copy = pltpu.make_async_copy(wk_hbm.at[layer], wk, w_sem.at[1])
    wv_copy = pltpu.make_async_copy(wv_hbm.at[layer], wv, w_sem.at[2])
    wo_copy = pltpu.make_async_copy(wo_hbm.at[layer], wo, w_sem.at[3])
    wk_copy.start()
    wv_copy.start()
    wq_copy.start()
    for i in range(min(ahead, blocks)):
        k_in(i).start()

    xbuf[...] = jnp.zeros_like(xbuf)
    xbuf[0:batch, :] = x_ref[...].astype(F32)
    normed = norm_rows(xbuf[...], gain_ref[layer, 0:1, :])

    row_id = lax.broadcasted_iota(jnp.int32, (8, HEAD), 0)
    pos_rows = jnp.full((8, HEAD), pos_ref[0], jnp.int32)
    for b in range(1, batch):
        pos_rows = jnp.where(row_id == b, pos_ref[b], pos_rows)
    angles = pos_rows.astype(F32) * freq_ref[...]
    lane_id = lax.broadcasted_iota(jnp.int32, (8, HEAD), 1)
    cos_part = jnp.cos(angles)
    sin_part = jnp.sin(angles)
    sin_part = jnp.where(lane_id < HEAD // 2, -sin_part, sin_part)

    wk_copy.wait()
    key_new = rotate(matmul(normed, wk[...]), cos_part, sin_part).astype(BF16)
    wv_copy.wait()
    value_new = matmul(normed, wv[...]).astype(BF16)
    wq_copy.wait()
    queries = matmul(normed, wq[...])
    stacked = jnp.concatenate([rotate(queries[:, h * HEAD:(h + 1) * HEAD], cos_part, sin_part)[0:4] for h in range(heads)], axis=0)
    rows = 4 * heads
    of_row = lax.broadcasted_iota(jnp.int32, (rows, HEAD), 0) % 4
    lhs = jnp.concatenate([jnp.where(of_row == b, stacked, 0.0) for b in range(batch)], axis=1).astype(BF16)

    slots = [pos_ref[b] % window if window else pos_ref[b] for b in range(batch)]
    tile_rows = lax.broadcasted_iota(jnp.int32, (16, HEAD), 0)

    def put_row(buf, new_rows, i):
        for b in range(batch):
            @pl.when(slots[b] // block == i)
            def _():
                base = pl.multiple_of((slots[b] // 16) * 16, 16)
                tile = buf[b, pl.ds(base, 16), :]
                new_row = jnp.broadcast_to(new_rows[b:b + 1, :].astype(F32), (16, HEAD))
                kept = tile.astype(F32)
                buf[b, pl.ds(base, 16), :] = jnp.where(tile_rows == slots[b] - base, new_row, kept).astype(BF16)

    col_ids = lax.broadcasted_iota(jnp.int32, (rows, block), 1)
    of_col = lax.broadcasted_iota(jnp.int32, (rows, block), 0) % 4
    limits = jnp.full((rows, block), pos_ref[0], jnp.int32)
    for b in range(1, batch):
        limits = jnp.where(of_col == b, pos_ref[b], limits)

    def score_step(i, total):
        k_in(i).wait()

        @pl.when(i + ahead < blocks)
        def _():
            k_in(i + ahead).start()

        @pl.when(i + ahead >= blocks)
        def _():
            v_in(i + ahead - blocks).start()

        @pl.when(i == max(blocks - ahead, 0))
        def _():
            wo_copy.start()

        put_row(kbuf, key_new, i)
        span = pl.ds(i * block, block)
        keys = jnp.concatenate([kbuf[b, span, :] for b in range(batch)], axis=1)
        logits = lax.dot_general(lhs, keys, (((1,), (1,)), ((), ())), preferred_element_type=F32) * HEAD ** -0.5
        weights = jnp.exp(SOFT_CAP * jnp.tanh(logits / SOFT_CAP))
        if not window:
            weights = jnp.where(col_ids + i * block <= limits, weights, 0.0)
        ebuf[i] = weights
        k_back(i).start()
        return total + jnp.sum(weights, axis=-1, keepdims=True)

    total = lax.fori_loop(0, blocks, score_step, jnp.zeros((rows, 1), F32))
    inv_total = 1.0 / total

    def value_step(i, acc):
        v_in(i).wait()

        @pl.when(i + ahead < blocks)
        def _():
            v_in(i + ahead).start()

        put_row(vbuf, value_new, i)
        span = pl.ds(i * block, block)
        values = jnp.concatenate([vbuf[b, span, :] for b in range(batch)], axis=1)
        probs = (ebuf[i] * inv_total).astype(BF16)
        out = acc + matmul(probs, values)
        v_back(i).start()
        return out

    mixed = lax.fori_loop(0, blocks, value_step, jnp.zeros((rows, batch * HEAD), F32))
    picked = jnp.zeros((rows, HEAD), F32)
    for b in range(batch):
        picked = jnp.where(of_row == b, mixed[:, b * HEAD:(b + 1) * HEAD], picked)
    merged = jnp.concatenate([picked[4 * h:4 * h + 4, :] for h in range(heads)], axis=1).astype(BF16)
    wo_copy.wait()
    o_ref[...] = matmul(merged, wo[...]).astype(BF16)

    def drain(i, carry):
        k_back(i).wait()
        v_back(i).wait()
        return carry

    lax.fori_loop(0, blocks, drain, 0)


def attn_call(layer, block, ahead, window, positions, freqs, hidden, gains, w_query, w_key, w_value, w_out, k_cache, v_cache):
    batch, length, head = k_cache.shape
    width, q_cols = w_query.shape[1:]
    blocks = length // block
    vmem = pl.BlockSpec(memory_space=pltpu.VMEM)
    hbm = pl.BlockSpec(memory_space=pl.ANY)
    smem = pl.BlockSpec(memory_space=pltpu.SMEM)
    cache = jax.ShapeDtypeStruct(k_cache.shape, k_cache.dtype)
    return pl.pallas_call(
        functools.partial(attn_kernel, layer, block, ahead, window),
        name=f"attn{layer}",
        out_shape=(jax.ShapeDtypeStruct((4, width), BF16), cache, cache),
        in_specs=[smem, vmem, vmem, vmem] + [hbm] * 6,
        out_specs=(vmem, hbm, hbm),
        scratch_shapes=[
            pltpu.VMEM(k_cache.shape, BF16),
            pltpu.VMEM(k_cache.shape, BF16),
            pltpu.VMEM((width, q_cols), BF16),
            pltpu.VMEM((width, head), BF16),
            pltpu.VMEM((width, head), BF16),
            pltpu.VMEM((q_cols, width), BF16),
            pltpu.VMEM((8, width), F32),
            pltpu.VMEM((blocks, 4 * q_cols // head, block), F32),
            pltpu.SemaphoreType.DMA((4,)),
            pltpu.SemaphoreType.DMA((blocks,)),
            pltpu.SemaphoreType.DMA((blocks,)),
            pltpu.SemaphoreType.DMA((blocks,)),
            pltpu.SemaphoreType.DMA((blocks,)),
        ],
        compiler_params=pltpu.CompilerParams(vmem_limit_bytes=(50 if layer else 58) * MIB),
    )(positions, freqs, hidden, gains, w_query, w_key, w_value, w_out, k_cache, v_cache)


def mlp_kernel(layer, n, row_chunks, col_chunks, o_ref, x_ref, gain_ref, wg_hbm, wu_hbm, wd_hbm, x_out,
               wg, wu, wd, part1, part2, acc_g, acc_u, g_sem, u_sem, d_sem, send1, recv1, send2, recv2):
    me = lax.axis_index("tp")
    batch, width = x_ref.shape
    ff = wg.shape[1]
    row_len = width // row_chunks
    col_len = width // col_chunks

    def g_in(i):
        rows = pl.ds(i * row_len, row_len)
        return pltpu.make_async_copy(wg_hbm.at[layer, rows, :], wg.at[rows, :], g_sem.at[i])

    def u_in(i):
        rows = pl.ds(i * row_len, row_len)
        return pltpu.make_async_copy(wu_hbm.at[layer, rows, :], wu.at[rows, :], u_sem.at[i])

    def d_in(i):
        cols = pl.ds(i * col_len, col_len)
        return pltpu.make_async_copy(wd_hbm.at[layer, :, cols], wd.at[:, cols], d_sem.at[i])

    for i in range(row_chunks):
        g_in(i).start()
        u_in(i).start()
    for i in range(col_chunks):
        d_in(i).start()

    barrier = pltpu.get_barrier_semaphore()
    peers = [lax.rem(me + k, n) for k in range(1, n)]
    for peer in peers:
        pl.semaphore_signal(barrier, inc=1, device_id={"tp": peer})
    pl.semaphore_wait(barrier, n - 1)

    def send(k, buf, cols, send_sem, recv_sem):
        return pltpu.make_async_remote_copy(
            src_ref=buf.at[me, :, cols], dst_ref=buf.at[me, :, cols], send_sem=send_sem, recv_sem=recv_sem,
            device_id={"tp": peers[k]})

    part1[me] = o_ref[...]
    all_cols = pl.ds(0, width)
    copies1 = [send(k, part1, all_cols, send1.at[k], recv1.at[k]) for k in range(n - 1)]
    for copy in copies1:
        copy.start()
    for copy in copies1:
        copy.wait_recv()

    def summed(buf):
        acc = buf[0].astype(F32)
        for j in range(1, n):
            acc = acc + buf[j].astype(F32)
        return acc[0:batch]

    gains = gain_ref[layer]
    normed = norm_rows(summed(part1), gains[1:2, :])
    mid = (x_ref[...].astype(F32) + normed.astype(F32)).astype(BF16)
    mid_f32 = mid.astype(F32)
    pre = norm_rows(mid_f32, gains[2:3, :])

    acc_g[...] = jnp.zeros_like(acc_g)
    acc_u[...] = jnp.zeros_like(acc_u)
    for i in range(row_chunks):
        rows = pl.ds(i * row_len, row_len)
        lhs = pre[:, i * row_len:(i + 1) * row_len]
        g_in(i).wait()
        acc_g[0:batch, :] += matmul(lhs, wg[rows, :])
        u_in(i).wait()
        acc_u[0:batch, :] += matmul(lhs, wu[rows, :])
    act = (jax.nn.gelu(acc_g[...], approximate=True) * acc_u[...]).astype(BF16)

    copies2 = []
    for i in range(col_chunks):
        cols = pl.ds(i * col_len, col_len)
        d_in(i).wait()
        down = matmul(act, wd[:, cols])
        part2[me, :, cols] = down[0:4].astype(BF16)
        for k in range(n - 1):
            copy = send(k, part2, cols, send2.at[i, k], recv2.at[i, k])
            copy.start()
            copies2.append(copy)
    for copy in copies2:
        copy.wait_recv()
    normed = norm_rows(summed(part2), gains[3:4, :])
    x_out[...] = (mid_f32 + normed.astype(F32)).astype(BF16)
    for copy in copies1 + copies2:
        copy.wait_send()


def mlp_call(layer, n, o_part, hidden, gains, w_gate, w_up, w_down):
    batch, width = hidden.shape
    ff = w_gate.shape[2]
    row_chunks, col_chunks = 8, 8
    vmem = pl.BlockSpec(memory_space=pltpu.VMEM)
    hbm = pl.BlockSpec(memory_space=pl.ANY)
    return pl.pallas_call(
        functools.partial(mlp_kernel, layer, n, row_chunks, col_chunks),
        name=f"mlp{layer}",
        out_shape=jax.ShapeDtypeStruct((batch, width), BF16),
        in_specs=[vmem, vmem, vmem, hbm, hbm, hbm],
        out_specs=vmem,
        scratch_shapes=[
            pltpu.VMEM((width, ff), BF16),
            pltpu.VMEM((width, ff), BF16),
            pltpu.VMEM((ff, width), BF16),
            pltpu.VMEM((n, 4, width), BF16),
            pltpu.VMEM((n, 4, width), BF16),
            pltpu.VMEM((8, ff), F32),
            pltpu.VMEM((8, ff), F32),
            pltpu.SemaphoreType.DMA((row_chunks,)),
            pltpu.SemaphoreType.DMA((row_chunks,)),
            pltpu.SemaphoreType.DMA((col_chunks,)),
            pltpu.SemaphoreType.DMA((n - 1,)),
            pltpu.SemaphoreType.DMA((n - 1,)),
            pltpu.SemaphoreType.DMA((col_chunks, n - 1)),
            pltpu.SemaphoreType.DMA((col_chunks, n - 1)),
        ],
        compiler_params=pltpu.CompilerParams(vmem_limit_bytes=50 * MIB, collective_id=layer, has_side_effects=True),
    )(o_part, hidden, gains, w_gate, w_up, w_down)


def decode_step(n, hidden, positions, k_local, v_local, k_global, v_global, w_query, w_key, w_value, w_out, w_gate, w_up, w_down, norm_scale):
    freqs = np.float32(ROPE_BASE) ** (np.float32(-2.0) * np.arange(HEAD // 2, dtype=np.float32) / np.float32(HEAD))
    freqs = jnp.asarray(np.concatenate([freqs, freqs])[None, :])
    flat = lambda cache: cache.reshape(cache.shape[0], cache.shape[1], HEAD)
    window = k_local.shape[1]
    o_part, k_loc, v_loc = attn_call(0, 1024, 4, window, positions, freqs, hidden, norm_scale, w_query, w_key, w_value, w_out, flat(k_local), flat(v_local))
    hidden = mlp_call(0, n, o_part, hidden, norm_scale, w_gate, w_up, w_down)
    o_part, k_glo, v_glo = attn_call(1, 2048, 6, 0, positions, freqs, hidden, norm_scale, w_query, w_key, w_value, w_out, flat(k_global), flat(v_global))
    hidden = mlp_call(1, n, o_part, hidden, norm_scale, w_gate, w_up, w_down)
    return (hidden, k_loc.reshape(k_local.shape), v_loc.reshape(v_local.shape), k_glo.reshape(k_global.shape), v_glo.reshape(v_global.shape))


def solution(mesh):
    row_spec = P('dp', None)
    cache_spec = P('dp', None, 'tp', None)
    col_split = P(None, None, 'tp')
    row_split = P(None, 'tp', None)
    in_specs = (row_spec, P('dp'), cache_spec, cache_spec, cache_spec, cache_spec, col_split, col_split, col_split, row_split, col_split, col_split, row_split, P())
    out_specs = (row_spec, cache_spec, cache_spec, cache_spec, cache_spec)
    body = functools.partial(decode_step, mesh.shape['tp'])
    return jax.shard_map(body, mesh=mesh, in_specs=in_specs, out_specs=out_specs, check_vma=False)
```

```python
import functools

import jax
import jax.numpy as jnp
import numpy as np
from jax import lax
from jax.experimental import pallas as pl
from jax.experimental.pallas import tpu as pltpu
from jax.sharding import PartitionSpec as P

SOFT_CAP = 50.0
NORM_EPS = 1e-6
ROPE_BASE = 10000.0
HEAD = 128
MIB = 1024 * 1024
AHEAD, EARLY1, EARLY2 = 99, 0, 0
F32 = jnp.float32
BF16 = jnp.bfloat16


def in_vmem(value):
    return pltpu.with_memory_space_constraint(value, pltpu.VMEM)


def in_hbm(value):
    return pltpu.with_memory_space_constraint(value, pltpu.HBM)


def norm_rows(values, gain_row):
    inv_rms = lax.rsqrt(jnp.mean(values * values, axis=-1, keepdims=True) + NORM_EPS)
    return (values * inv_rms * (1.0 + gain_row)).astype(BF16)


def matmul(lhs, rhs):
    return jnp.dot(lhs, rhs, preferred_element_type=F32)


def rotate(head, cos_part, sin_part):
    return head * cos_part + pltpu.roll(head, HEAD // 2, 1) * sin_part


def attn_kernel(layer, block, window, k_kept, pos_hbm, freq_hbm, x_in, gain_hbm, wq_hbm, wk_hbm, wv_hbm, wo_hbm, k_in, v_hbm,
                o_ref, k_out, v_out, *scratch):
    if k_kept:
        kbuf = k_in
        scratch = scratch[:7] + (x_in,) + scratch[7:]
    else:
        kbuf, scratch = scratch[0], scratch[1:]
    vbuf, wq, wk, wv, wo, pos_ref, freq_ref, x_ref, gain_ref, xbuf, ebuf, tiles, load_sem, t_sem, kout_sem, vout_sem = scratch
    batch, length = v_hbm.shape[0], v_hbm.shape[1]
    heads = wq.shape[1] // HEAD
    blocks = length // block

    def piece(i):
        return pl.ds(pl.multiple_of(i * block, block), block)

    def k_load(i):
        return pltpu.make_async_copy(k_in.at[:, piece(i), :], kbuf.at[:, piece(i), :], load_sem.at[8 + i])

    def v_load(i):
        return pltpu.make_async_copy(v_hbm.at[:, piece(i), :], vbuf.at[:, piece(i), :], load_sem.at[8 + blocks + i])

    def k_back(i):
        return pltpu.make_async_copy(kbuf.at[:, piece(i), :], k_out.at[:, piece(i), :], kout_sem.at[i])

    def v_back(i):
        return pltpu.make_async_copy(vbuf.at[:, piece(i), :], v_out.at[:, piece(i), :], vout_sem.at[i])

    pos_copy = pltpu.make_async_copy(pos_hbm, pos_ref, load_sem.at[0])
    freq_copy = pltpu.make_async_copy(freq_hbm, freq_ref, load_sem.at[1])
    if not k_kept:
        x_copy = pltpu.make_async_copy(x_in, x_ref, load_sem.at[2])
    gain_copy = pltpu.make_async_copy(gain_hbm.at[layer], gain_ref, load_sem.at[3])
    wq_copy = pltpu.make_async_copy(wq_hbm.at[layer], wq, load_sem.at[4])
    wk_copy = pltpu.make_async_copy(wk_hbm.at[layer], wk, load_sem.at[5])
    wv_copy = pltpu.make_async_copy(wv_hbm.at[layer], wv, load_sem.at[6])
    wo_copy = pltpu.make_async_copy(wo_hbm.at[layer], wo, load_sem.at[7])
    first = (gain_copy, pos_copy, freq_copy, wk_copy, wq_copy, wv_copy)
    for copy in first if k_kept else (x_copy,) + first:
        copy.start()
    if not k_kept:
        for i in range(blocks):
            k_load(i).start()
    for i in range(blocks):
        v_load(i).start()
    wo_copy.start()

    xbuf[...] = jnp.zeros_like(xbuf)
    if not k_kept:
        x_copy.wait()
    gain_copy.wait()
    xbuf[0:batch, :] = x_ref[...].astype(F32)
    normed = norm_rows(xbuf[...], gain_ref[0:1, :])

    pos_copy.wait()
    freq_copy.wait()
    row_id = lax.broadcasted_iota(jnp.int32, (8, HEAD), 0)
    pos_rows = jnp.full((8, HEAD), pos_ref[0], jnp.int32)
    for b in range(1, batch):
        pos_rows = jnp.where(row_id == b, pos_ref[b], pos_rows)
    angles = pos_rows.astype(F32) * freq_ref[...]
    lane_id = lax.broadcasted_iota(jnp.int32, (8, HEAD), 1)
    cos_part = jnp.cos(angles)
    sin_part = jnp.sin(angles)
    sin_part = jnp.where(lane_id < HEAD // 2, -sin_part, sin_part)

    wk_copy.wait()
    key_new = rotate(matmul(normed, wk[...]), cos_part, sin_part).astype(BF16)
    wq_copy.wait()
    queries = matmul(normed, wq[...])
    stacked = jnp.concatenate([rotate(queries[:, h * HEAD:(h + 1) * HEAD], cos_part, sin_part)[0:4] for h in range(heads)], axis=0)
    rows = 4 * heads
    of_row = lax.broadcasted_iota(jnp.int32, (rows, HEAD), 0) % 4
    lhs = jnp.concatenate([jnp.where(of_row == b, stacked, 0.0) for b in range(batch)], axis=1).astype(BF16)
    wv_copy.wait()
    if k_kept:
        for i in range(blocks):
            k_back(i).start()
    value_new = matmul(normed, wv[...]).astype(BF16)

    slots = [pos_ref[b] % window if window else pos_ref[b] for b in range(batch)]
    tile_rows = lax.broadcasted_iota(jnp.int32, (16, HEAD), 0)

    def put_row(buf, new_rows, i):
        for b in range(batch):
            @pl.when(slots[b] // block == i)
            def _():
                base = pl.multiple_of((slots[b] // 16) * 16, 16)
                tile = buf[b, pl.ds(base, 16), :]
                new_row = jnp.broadcast_to(new_rows[b:b + 1, :].astype(F32), (16, HEAD))
                kept = tile.astype(F32)
                buf[b, pl.ds(base, 16), :] = jnp.where(tile_rows == slots[b] - base, new_row, kept).astype(BF16)

    if k_kept:
        key_rows = jnp.concatenate([key_new[0:4]] * heads, axis=0).astype(F32)
        new_logits = jnp.sum(stacked.astype(BF16).astype(F32) * key_rows, axis=-1, keepdims=True) * HEAD ** -0.5
        new_weights = jnp.exp(SOFT_CAP * jnp.tanh(new_logits / SOFT_CAP))

    col_ids = lax.broadcasted_iota(jnp.int32, (rows, block), 1)
    of_col = lax.broadcasted_iota(jnp.int32, (rows, block), 0) % 4
    limits = jnp.full((rows, block), pos_ref[0], jnp.int32)
    for b in range(1, batch):
        limits = jnp.where(of_col == b, pos_ref[b], limits)

    def score_step(i, total):
        if not k_kept:
            k_load(i).wait()
            put_row(kbuf, key_new, i)
        keys = jnp.concatenate([kbuf[b, piece(i), :] for b in range(batch)], axis=1)
        logits = lax.dot_general(lhs, keys, (((1,), (1,)), ((), ())), preferred_element_type=F32) * HEAD ** -0.5
        weights = jnp.exp(SOFT_CAP * jnp.tanh(logits / SOFT_CAP))
        if k_kept:
            col_pos = col_ids + i * block
            weights = jnp.where(col_pos < limits, weights, jnp.where(col_pos == limits, new_weights, 0.0))
        ebuf[i] = weights
        if not k_kept:
            k_back(i).start()
        return total + jnp.sum(weights, axis=-1, keepdims=True)

    total = lax.fori_loop(0, blocks, score_step, jnp.zeros((rows, 1), F32))
    inv_total = 1.0 / total

    def value_step(i, acc):
        v_load(i).wait()
        put_row(vbuf, value_new, i)
        values = jnp.concatenate([vbuf[b, piece(i), :] for b in range(batch)], axis=1)
        probs = (ebuf[i] * inv_total).astype(BF16)
        out = acc + matmul(probs, values)
        v_back(i).start()
        return out

    mixed = lax.fori_loop(0, blocks, value_step, jnp.zeros((rows, batch * HEAD), F32))
    tile_copies = []
    if k_kept:
        for i in range(blocks):
            k_back(i).wait()
        for b in range(batch):
            base = pl.multiple_of((slots[b] // 16) * 16, 16)
            tile = kbuf[b, pl.ds(base, 16), :].astype(F32)
            new_row = jnp.broadcast_to(key_new[b:b + 1, :].astype(F32), (16, HEAD))
            tiles[b] = jnp.where(tile_rows == slots[b] - base, new_row, tile).astype(BF16)
            tile_copies.append(pltpu.make_async_copy(tiles.at[b], k_out.at[b, pl.ds(base, 16), :], t_sem.at[b]))
    picked = jnp.zeros((rows, HEAD), F32)
    for b in range(batch):
        picked = jnp.where(of_row == b, mixed[:, b * HEAD:(b + 1) * HEAD], picked)
    merged = jnp.concatenate([picked[4 * h:4 * h + 4, :] for h in range(heads)], axis=1).astype(BF16)
    for copy in tile_copies:
        copy.start()
    wo_copy.wait()
    o_ref[...] = matmul(merged, wo[...]).astype(BF16)

    def drain(i, carry):
        if not k_kept:
            k_back(i).wait()
        v_back(i).wait()
        return carry

    lax.fori_loop(0, blocks, drain, 0)
    for copy in tile_copies:
        copy.wait()


def attn_call(layer, block, window, k_kept, positions, freqs, hidden, gains, w_query, w_key, w_value, w_out, k_cache, v_cache):
    batch, length, head = v_cache.shape
    width, q_cols = w_query.shape[1:]
    blocks = length // block
    vmem = pl.BlockSpec(memory_space=pltpu.VMEM)
    hbm = pl.BlockSpec(memory_space=pl.ANY)
    cache = jax.ShapeDtypeStruct(v_cache.shape, v_cache.dtype)
    kbuf = [] if k_kept else [pltpu.VMEM(v_cache.shape, BF16)]
    return pl.pallas_call(
        functools.partial(attn_kernel, layer, block, window, k_kept),
        name=f"attn{layer}",
        out_shape=(pltpu.VMEM((4, width), BF16), cache, cache),
        in_specs=[hbm, hbm, vmem if k_kept else hbm] + [hbm] * 5 + [vmem if k_kept else hbm, hbm],
        out_specs=(vmem, hbm, hbm),
        scratch_shapes=kbuf + [
            pltpu.VMEM(v_cache.shape, BF16),
            pltpu.VMEM((width, q_cols), BF16),
            pltpu.VMEM((width, head), BF16),
            pltpu.VMEM((width, head), BF16),
            pltpu.VMEM((q_cols, width), BF16),
            pltpu.SMEM((batch,), jnp.int32),
            pltpu.VMEM((1, head), F32),
        ] + ([] if k_kept else [pltpu.VMEM((batch, width), BF16)]) + [
            pltpu.VMEM((4, width), F32),
            pltpu.VMEM((8, width), F32),
            pltpu.VMEM((blocks, 4 * q_cols // head, block), F32),
            pltpu.VMEM((batch, 16, head), BF16),
            pltpu.SemaphoreType.DMA((8 + 2 * blocks,)),
            pltpu.SemaphoreType.DMA((batch,)),
            pltpu.SemaphoreType.DMA((blocks,)),
            pltpu.SemaphoreType.DMA((blocks,)),
        ],
        compiler_params=pltpu.CompilerParams(vmem_limit_bytes=int((45 if layer else 60) * MIB)),
    )(*(in_hbm(value) for value in (positions, freqs)), (in_vmem if k_kept else in_hbm)(hidden),
      *(in_hbm(value) for value in (gains, w_query, w_key, w_value, w_out)), (in_vmem if k_kept else in_hbm)(k_cache), in_hbm(v_cache))


def mlp_kernel(layer, n, row_chunks, col_chunks, k_pieces, o_ref, x_in, gain_hbm, wg_hbm, wu_hbm, wd_hbm, *refs):
    if k_pieces:
        k_hbm, x_out, k_pre = refs[:3]
        refs = refs[3:]
    else:
        x_out, refs = refs[0], refs[1:]
    if layer:
        x_ref = x_in
    else:
        x_ref, refs = refs[0], refs[1:]
    wg, wu, wd, gain_ref, part1, part2, acc_g, acc_u, load_sem, send1, recv1, send2, recv2 = refs
    me = lax.axis_index("tp")
    batch, width = x_ref.shape
    row_len = width // row_chunks
    col_len = width // col_chunks
    row_dots, col_dots, ahead, early1, early2 = 2, 4, AHEAD, EARLY1, EARLY2

    def g_in(i):
        rows = pl.ds(i * row_len, row_len)
        return pltpu.make_async_copy(wg_hbm.at[layer, rows, :], wg.at[rows, :], load_sem.at[2 + i])

    def u_in(i):
        rows = pl.ds(i * row_len, row_len)
        return pltpu.make_async_copy(wu_hbm.at[layer, rows, :], wu.at[rows, :], load_sem.at[2 + row_chunks + i])

    def d_in(i):
        cols = pl.ds(i * col_len, col_len)
        return pltpu.make_async_copy(wd_hbm.at[layer, :, cols], wd.at[:, cols], load_sem.at[2 + 2 * row_chunks + i])

    if not layer:
        x_copy = pltpu.make_async_copy(x_in, x_ref, load_sem.at[0])
    gain_copy = pltpu.make_async_copy(gain_hbm.at[layer], gain_ref, load_sem.at[1])
    k_copies = []
    for i in range(k_pieces):
        k_len = k_hbm.shape[1] // k_pieces
        slots = pl.ds(i * k_len, k_len)
        k_copies.append(pltpu.make_async_copy(k_hbm.at[:, slots, :], k_pre.at[:, slots, :], load_sem.at[2 + 2 * row_chunks + col_chunks + i]))
    loads = []
    for d in range(row_dots):
        span = range(d * row_chunks // row_dots, (d + 1) * row_chunks // row_dots)
        loads += [g_in(i) for i in span] + [u_in(i) for i in span]
    loads += [d_in(i) for i in range(col_chunks)] + k_copies
    arrived = 0

    def wait_loads(count):
        nonlocal arrived
        while arrived < min(count, len(loads)):
            loads[arrived].wait()
            if arrived + ahead < len(loads):
                loads[arrived + ahead].start()
            arrived += 1

    if not layer:
        x_copy.start()
    gain_copy.start()
    for load in loads[:ahead]:
        load.start()

    barrier = pltpu.get_barrier_semaphore()
    peers = [lax.rem(me // 4 + far // 4, 2) * 4 + lax.rem(me // 2 + far // 2, 2) * 2 + lax.rem(me + far, 2) for far in (6, 7, 4, 5, 2, 3, 1)]
    for peer in peers:
        pl.semaphore_signal(barrier, inc=1, device_id={"tp": peer})
    pl.semaphore_wait(barrier, n - 1)

    def send(k, buf, cols, send_sem, recv_sem):
        return pltpu.make_async_remote_copy(
            src_ref=buf.at[me, :, cols], dst_ref=buf.at[me, :, cols], send_sem=send_sem, recv_sem=recv_sem,
            device_id={"tp": peers[k]})

    part1[me] = o_ref[...]
    all_cols = pl.ds(0, width)
    copies1 = [send(k, part1, all_cols, send1.at[k], recv1.at[k]) for k in range(n - 1)]
    for copy in copies1:
        copy.start()
    if not layer:
        x_copy.wait()
    gain_copy.wait()
    wait_loads(early1)
    for copy in copies1:
        copy.wait_recv()

    def summed(buf):
        acc = buf[0].astype(F32)
        for j in range(1, n):
            acc = acc + buf[j].astype(F32)
        return acc[0:batch]

    normed = norm_rows(summed(part1), gain_ref[1:2, :])
    mid = (x_ref[...].astype(F32) + normed.astype(F32)).astype(BF16)
    mid_f32 = mid.astype(F32)
    pre = norm_rows(mid_f32, gain_ref[2:3, :])

    for d in range(row_dots):
        first, last = d * row_chunks // row_dots, (d + 1) * row_chunks // row_dots
        rows = slice(first * row_len, last * row_len)
        lhs = pre[:, rows]
        wait_loads(first + last)
        gate = matmul(lhs, wg[rows, :])
        acc_g[0:batch, :] = gate if d == 0 else acc_g[0:batch, :] + gate
        wait_loads(2 * last)
        up = matmul(lhs, wu[rows, :])
        acc_u[0:batch, :] = up if d == 0 else acc_u[0:batch, :] + up
    act = (jax.nn.gelu(acc_g[0:batch, :], approximate=True) * acc_u[0:batch, :]).astype(BF16)

    copies2 = []
    for d in range(col_dots):
        first, last = d * col_chunks // col_dots, (d + 1) * col_chunks // col_dots
        wait_loads(2 * row_chunks + last)
        down = matmul(act, wd[:, first * col_len:last * col_len])
        cols = pl.ds(first * col_len, (last - first) * col_len)
        part2[me, 0:batch, cols] = down.astype(BF16)
        for k in range(n - 1):
            copy = send(k, part2, cols, send2.at[d, k], recv2.at[d, k])
            copy.start()
            copies2.append(copy)
    wait_loads(2 * row_chunks + col_chunks + early2)
    for copy in copies2:
        copy.wait_recv()
    normed = norm_rows(summed(part2), gain_ref[3:4, :])
    x_out[...] = (mid_f32 + normed.astype(F32)).astype(BF16)
    for copy in copies1 + copies2:
        copy.wait_send()
    wait_loads(len(loads))


def mlp_call(layer, n, k_pieces, o_part, hidden, gains, w_gate, w_up, w_down, *k_cache):
    batch, width = hidden.shape
    ff = w_gate.shape[2]
    row_chunks, col_chunks = 8, 8
    vmem = pl.BlockSpec(memory_space=pltpu.VMEM)
    hbm = pl.BlockSpec(memory_space=pl.ANY)
    kept = tuple(pltpu.VMEM(cache.shape, cache.dtype) for cache in k_cache)
    return pl.pallas_call(
        functools.partial(mlp_kernel, layer, n, row_chunks, col_chunks, k_pieces),
        name=f"mlp{layer}",
        out_shape=((jax.ShapeDtypeStruct if layer else pltpu.VMEM)((batch, width), BF16),) + kept,
        in_specs=[vmem, vmem if layer else hbm] + [hbm] * (4 + len(kept)),
        out_specs=(vmem,) * (1 + len(kept)),
        scratch_shapes=([] if layer else [pltpu.VMEM((batch, width), BF16)]) + [
            pltpu.VMEM((width, ff), BF16),
            pltpu.VMEM((width, ff), BF16),
            pltpu.VMEM((ff, width), BF16),
            pltpu.VMEM((4, width), F32),
            pltpu.VMEM((n, 4, width), BF16),
            pltpu.VMEM((n, 4, width), BF16),
            pltpu.VMEM((8, ff), F32),
            pltpu.VMEM((8, ff), F32),
            pltpu.SemaphoreType.DMA((2 + 2 * row_chunks + col_chunks + k_pieces,)),
            pltpu.SemaphoreType.DMA((n - 1,)),
            pltpu.SemaphoreType.DMA((n - 1,)),
            pltpu.SemaphoreType.DMA((col_chunks, n - 1)),
            pltpu.SemaphoreType.DMA((col_chunks, n - 1)),
        ],
        compiler_params=pltpu.CompilerParams(vmem_limit_bytes=int(44 * MIB), collective_id=layer, has_side_effects=True),
    )(in_vmem(o_part), (in_vmem if layer else in_hbm)(hidden), *(in_hbm(value) for value in (gains, w_gate, w_up, w_down) + k_cache))


def decode_step(n, hidden, positions, k_local, v_local, k_global, v_global, w_query, w_key, w_value, w_out, w_gate, w_up, w_down, norm_scale):
    freqs = np.float32(ROPE_BASE) ** (np.float32(-2.0) * np.arange(HEAD // 2, dtype=np.float32) / np.float32(HEAD))
    freqs = jnp.asarray(np.concatenate([freqs, freqs])[None, :])
    flat = lambda cache: cache.reshape(cache.shape[0], cache.shape[1], HEAD)
    window = k_local.shape[1]
    shared = (positions, freqs)
    weights = (norm_scale, w_query, w_key, w_value, w_out)
    o_part, k_loc, v_loc = attn_call(0, 2048, window, False, *shared, hidden, *weights, flat(k_local), flat(v_local))
    hidden, k_pre = mlp_call(0, n, 12, o_part, hidden, norm_scale, w_gate, w_up, w_down, flat(k_global))
    o_part, k_glo, v_glo = attn_call(1, 4096, 0, True, *shared, hidden, *weights, k_pre, flat(v_global))
    hidden, = mlp_call(1, n, 0, o_part, hidden, norm_scale, w_gate, w_up, w_down)
    return (hidden, k_loc.reshape(k_local.shape), v_loc.reshape(v_local.shape), k_glo.reshape(k_global.shape), v_glo.reshape(v_global.shape))


def solution(mesh):
    row_spec = P('dp', None)
    cache_spec = P('dp', None, 'tp', None)
    col_split = P(None, None, 'tp')
    row_split = P(None, 'tp', None)
    in_specs = (row_spec, P('dp'), cache_spec, cache_spec, cache_spec, cache_spec, col_split, col_split, col_split, row_split, col_split, col_split, row_split, P())
    out_specs = (row_spec, cache_spec, cache_spec, cache_spec, cache_spec)
    body = functools.partial(decode_step, mesh.shape['tp'])
    return jax.shard_map(body, mesh=mesh, in_specs=in_specs, out_specs=out_specs, check_vma=False)
```

```python
import functools

import jax
import jax.numpy as jnp
import numpy as np
from jax import lax
from jax.experimental import pallas as pl
from jax.experimental.pallas import tpu as pltpu
from jax.sharding import PartitionSpec as P

SOFT_CAP = 50.0
NORM_EPS = 1e-6
ROPE_BASE = 10000.0
HEAD = 128
MIB = 1024 * 1024
F32 = jnp.float32
BF16 = jnp.bfloat16
ROW_CHUNKS, ROW_DOTS = 8, 2
COL_CHUNKS, COL_DOTS = 8, 4
K_EARLY = 4
K_PIECES = 12
LOCAL_BLOCKS = 2
LAYER0_MIB, ATTN_MIB = 32, 32
QKV_CHUNKS = 4
COPY = pltpu.make_async_copy


def in_vmem(value):
    return pltpu.with_memory_space_constraint(value, pltpu.VMEM)


def in_hbm(value):
    return pltpu.with_memory_space_constraint(value, pltpu.HBM)


def norm_rows(values, gain_row):
    inv_rms = lax.rsqrt(jnp.mean(values * values, axis=-1, keepdims=True) + NORM_EPS)
    return (values * inv_rms * (1.0 + gain_row)).astype(BF16)


def matmul(lhs, rhs):
    return jnp.dot(lhs, rhs, preferred_element_type=F32)


def capped_exp(logits):
    return jnp.exp(SOFT_CAP * jnp.tanh(logits * HEAD ** -0.5 / SOFT_CAP))


def rotate(head, cos_part, sin_part):
    return head * cos_part + pltpu.roll(head, HEAD // 2, 1) * sin_part


def rope_tables(pos_ref, freq_ref, batch):
    row_id = lax.broadcasted_iota(jnp.int32, (8, HEAD), 0)
    pos_rows = jnp.full((8, HEAD), pos_ref[0], jnp.int32)
    for b in range(1, batch):
        pos_rows = jnp.where(row_id == b, pos_ref[b], pos_rows)
    angles = pos_rows.astype(F32) * freq_ref[...]
    lane_id = lax.broadcasted_iota(jnp.int32, (8, HEAD), 1)
    sin_part = jnp.sin(angles)
    return jnp.cos(angles), jnp.where(lane_id < HEAD // 2, -sin_part, sin_part)


def row_of(rows):
    return lax.broadcasted_iota(jnp.int32, (rows, HEAD), 0) % 4


def stack_queries(queries, tables, heads, batch):
    stacked = jnp.concatenate([rotate(queries[:, h * HEAD:(h + 1) * HEAD], *tables)[0:4] for h in range(heads)], axis=0)
    of_row = row_of(4 * heads)
    lhs = jnp.concatenate([jnp.where(of_row == b, stacked, 0.0) for b in range(batch)], axis=1).astype(BF16)
    return stacked.astype(BF16).astype(F32), lhs


def per_head(new_rows, heads):
    return jnp.concatenate([new_rows[0:4]] * heads, axis=0).astype(F32)


def row_values(values, rows, cols):
    of_col = lax.broadcasted_iota(jnp.int32, (rows, cols), 0) % 4
    out = jnp.full((rows, cols), values[0], jnp.int32)
    for b in range(1, len(values)):
        out = jnp.where(of_col == b, values[b], out)
    return out


def pick_rows(mixed, heads, batch):
    of_row = row_of(4 * heads)
    picked = jnp.zeros((4 * heads, HEAD), F32)
    for b in range(batch):
        picked = jnp.where(of_row == b, mixed[:, b * HEAD:(b + 1) * HEAD], picked)
    return picked


def merge_heads(picked, heads):
    return jnp.concatenate([picked[4 * h:4 * h + 4, :] for h in range(heads)], axis=1).astype(BF16)


def score_rows(lhs, keys):
    return lax.dot_general(lhs, keys, (((1,), (1,)), ((), ())), preferred_element_type=F32)


class Loads:
    def __init__(self, sem):
        self.sem, self.count = sem, 0

    def add(self, src, dst):
        self.count += 1
        return COPY(src, dst, self.sem.at[self.count - 1])


def start_all(copies):
    for copy in copies:
        copy.start()


def wait_all(copies):
    for copy in copies:
        copy.wait()


class Exchange:
    def __init__(self, n, me, buf, send_sem, recv_sem):
        self.me, self.n, self.buf, self.send_sem, self.recv_sem = me, n, buf, send_sem, recv_sem
        self.peers = [lax.rem(me // 4 + far // 4, 2) * 4 + lax.rem(me // 2 + far // 2, 2) * 2 + lax.rem(me + far, 2) for far in (6, 7, 4, 5, 2, 3, 1)]
        self.sent = []

    def send(self, first, last):
        cols, i, group = pl.ds(first, last - first), len(self.sent), []
        for k, peer in enumerate(self.peers):
            group.append(pltpu.make_async_remote_copy(
                src_ref=self.buf.at[self.me, :, cols], dst_ref=self.buf.at[self.me, :, cols],
                send_sem=self.send_sem.at[i, k], recv_sem=self.recv_sem.at[i, k], device_id={"tp": peer}))
            group[k].start()
        self.sent.append((group, first, last))

    def summed(self, batch):
        parts = []
        for group, first, last in self.sent:
            for copy in group:
                copy.wait_recv()
            acc = self.buf[0, :, first:last].astype(F32)
            for j in range(1, self.n):
                acc = acc + self.buf[j, :, first:last].astype(F32)
            parts.append(acc)
        return jnp.concatenate(parts, axis=1)[0:batch]

    def drain(self):
        for group, _, _ in self.sent:
            for copy in group:
                copy.wait_send()


def row_loads(loads, hbm, layer, buf):
    step = buf.shape[0] // ROW_CHUNKS
    return [loads.add(hbm.at[layer, pl.ds(i * step, step), :], buf.at[pl.ds(i * step, step), :]) for i in range(ROW_CHUNKS)]


def mlp_tail(branch, hidden, gain_ref, gate, up, order, after, down_dots, wg, wu, acc_g, acc_u, exchange):
    batch, width = hidden.shape
    mid = (hidden + norm_rows(branch, gain_ref[1:2, :]).astype(F32)).astype(BF16).astype(F32)
    pre = norm_rows(mid, gain_ref[2:3, :])
    part = ROW_CHUNKS // ROW_DOTS
    row_len = width // ROW_DOTS
    for kind, d in order:
        loads, weights, acc = (gate, wg, acc_g) if kind == 0 else (up, wu, acc_u)
        wait_all(loads[d * part:(d + 1) * part])
        rows = slice(d * row_len, (d + 1) * row_len)
        product = matmul(pre[:, rows], weights[rows, :])
        acc[0:batch, :] = product if d == 0 else acc[0:batch, :] + product
        start_all(after.get((kind, d), []))
    act = (jax.nn.gelu(acc_g[0:batch, :], approximate=True) * acc_u[0:batch, :]).astype(BF16)
    first = 0
    for loads, buf, row, col, cols in down_dots:
        wait_all(loads)
        last = first + cols
        exchange.buf[exchange.me, 0:batch, first:last] = matmul(act, buf[row:row + act.shape[1], col:col + cols]).astype(BF16)
        exchange.send(first, last)
        first = last
    total = exchange.summed(batch)
    return (mid + norm_rows(total, gain_ref[3:4, :]).astype(F32)).astype(BF16)


def greet(exchange):
    barrier = pltpu.get_barrier_semaphore()
    for peer in exchange.peers:
        pl.semaphore_signal(barrier, inc=1, device_id={"tp": peer})
    return lambda: pl.semaphore_wait(barrier, exchange.n - 1)


def layer0_kernel(n, pos_hbm, freq_hbm, x_in, gain_hbm, wq_hbm, wk_hbm, wv_hbm, wo_hbm, k_hbm, v_hbm, wg_hbm, wu_hbm, wd_hbm, kg_hbm,
                  x_out, new_out, k_pre, kl_keep, vl_keep, wo_next, wg, wu, pos_ref, freq_ref, x_ref, gain_ref, xbuf, ebuf, part1, part2, acc_g, acc_u,
                  load_sem, send1, recv1, send2, recv2):
    me = lax.axis_index("tp")
    batch, width = x_in.shape
    window = k_hbm.shape[1]
    q_cols = wq_hbm.shape[2]
    heads = q_cols // HEAD
    half = width // 2
    first_ex, second_ex = Exchange(n, me, part1, send1, recv1), Exchange(n, me, part2, send2, recv2)
    loads = Loads(load_sem)
    small = [loads.add(x_in, x_ref), loads.add(gain_hbm.at[0], gain_ref), loads.add(pos_hbm, pos_ref), loads.add(freq_hbm, freq_ref)]
    qkv = []
    step = width // QKV_CHUNKS
    for h in range(QKV_CHUNKS):
        rows = pl.ds(h * step, step)
        qkv.append([loads.add(wk_hbm.at[0, rows, :], wu.at[rows, pl.ds(q_cols, HEAD)]),
                    loads.add(wv_hbm.at[0, rows, :], wu.at[rows, pl.ds(q_cols + HEAD, HEAD)]),
                    loads.add(wq_hbm.at[0, rows, :], wu.at[rows, pl.ds(0, q_cols)])])
    k_copy, v_copy = loads.add(k_hbm, kl_keep), loads.add(v_hbm, vl_keep)
    wo_copy, wo_again = loads.add(wo_hbm.at[0], wo_next), loads.add(wo_hbm.at[1], wo_next)
    gate, up = row_loads(loads, wg_hbm, 0, wg), row_loads(loads, wu_hbm, 0, wu)
    ff, col_len = wg.shape[1], width // COL_CHUNKS
    places = [(buf, row, col * col_len) for buf, row in ((wg, 0), (wg, ff), (wu, 0)) for col in range(3)][0:COL_CHUNKS]
    down = [loads.add(wd_hbm.at[0, :, pl.ds(i * col_len, col_len)], buf.at[pl.ds(row, ff), pl.ds(col, col_len)]) for i, (buf, row, col) in enumerate(places)]
    down_dots = [(down[i:i + count], *places[i], count * col_len) for i, count in ((0, 3), (3, 3), (6, 1), (7, 1))]
    k_len = kg_hbm.shape[1] // K_PIECES
    k_loads = [loads.add(kg_hbm.at[:, pl.ds(i * k_len, k_len), :], k_pre.at[:, pl.ds(i * k_len, k_len), :]) for i in range(K_PIECES)]
    start_all(small + sum(qkv, []) + [k_copy, v_copy, wo_copy] + gate)
    met = greet(first_ex)

    wait_all(small)
    xbuf[...] = jnp.zeros_like(xbuf)
    xbuf[0:batch, :] = x_ref[...].astype(F32)
    normed = norm_rows(xbuf[...], gain_ref[0:1, :])
    tables = rope_tables(pos_ref, freq_ref, batch)
    joint = jnp.zeros((8, q_cols + 2 * HEAD), F32)
    for h in range(QKV_CHUNKS):
        wait_all(qkv[h])
        span = slice(h * step, (h + 1) * step)
        joint = joint + matmul(normed[:, span], wu[span, 0:q_cols + 2 * HEAD])
    start_all(up)
    key_new = rotate(joint[:, q_cols:q_cols + HEAD], *tables).astype(BF16)
    value_new = joint[:, q_cols + HEAD:q_cols + 2 * HEAD].astype(BF16)
    new_out[0] = key_new
    new_out[1] = value_new
    stacked, lhs = stack_queries(joint[:, 0:q_cols], tables, heads, batch)
    new_weights = capped_exp(jnp.sum(stacked * per_head(key_new, heads), axis=-1, keepdims=True))

    rows = 4 * heads
    block = window // LOCAL_BLOCKS
    slots = row_values([pos_ref[b] % window for b in range(batch)], rows, block)
    col_ids = lax.broadcasted_iota(jnp.int32, (rows, block), 1)

    def score_step(i, total):
        span = pl.ds(pl.multiple_of(i * block, block), block)
        keys = jnp.concatenate([kl_keep[b, span, :] for b in range(batch)], axis=1)
        weights = capped_exp(score_rows(lhs, keys))
        weights = jnp.where(col_ids + i * block == slots, 0.0, weights)
        ebuf[i] = weights
        return total + jnp.sum(weights, axis=-1, keepdims=True)

    def value_step(i, acc):
        span = pl.ds(pl.multiple_of(i * block, block), block)
        values = jnp.concatenate([vl_keep[b, span, :] for b in range(batch)], axis=1)
        return acc + matmul((ebuf[i] * inv_total).astype(BF16), values)

    k_copy.wait()
    inv_total = 1.0 / lax.fori_loop(0, LOCAL_BLOCKS, score_step, new_weights)
    v_copy.wait()
    mixed = lax.fori_loop(0, LOCAL_BLOCKS, value_step, jnp.zeros((rows, batch * HEAD), F32))
    new_probs = (new_weights * inv_total).astype(BF16).astype(F32)
    merged = merge_heads(pick_rows(mixed, heads, batch) + new_probs * per_head(value_new, heads), heads)

    met()
    wo_copy.wait()
    for h in range(2):
        part1[me, :, h * half:(h + 1) * half] = matmul(merged, wo_next[:, h * half:(h + 1) * half]).astype(BF16)
        first_ex.send(h * half, (h + 1) * half)
    start_all(k_loads[:K_EARLY])
    hidden = x_ref[...].astype(F32)
    order = ((0, 0), (0, 1), (1, 0), (1, 1))
    after = {(0, 1): down[:6], (1, 0): down[6:] + k_loads[K_EARLY:] + [wo_again]}
    x_out[...] = mlp_tail(first_ex.summed(batch), hidden, gain_ref, gate, up, order, after, down_dots, wg, wu, acc_g, acc_u, second_ex)
    first_ex.drain()
    second_ex.drain()
    wait_all(k_loads + [wo_again])


def layer0_call(n, positions, freqs, hidden, gains, w_query, w_key, w_value, w_out, k_local, v_local, w_gate, w_up, w_down, k_global):
    batch, width = hidden.shape
    ff = w_gate.shape[2]
    hbm = pl.BlockSpec(memory_space=pl.ANY)
    vmem = pl.BlockSpec(memory_space=pltpu.VMEM)
    args = (positions, freqs, hidden, gains, w_query, w_key, w_value, w_out, k_local, v_local, w_gate, w_up, w_down, k_global)
    return pl.pallas_call(
        functools.partial(layer0_kernel, n),
        name="layer0",
        out_shape=(pltpu.VMEM((batch, width), BF16), pltpu.VMEM((2, 8, HEAD), BF16), pltpu.VMEM(k_global.shape, BF16),
                   pltpu.VMEM(k_local.shape, BF16), pltpu.VMEM(v_local.shape, BF16), pltpu.VMEM(w_out.shape[1:], BF16)),
        in_specs=[hbm] * len(args),
        out_specs=(vmem,) * 6,
        scratch_shapes=[
            pltpu.VMEM((width, ff), BF16),
            pltpu.VMEM((width, ff), BF16),
            pltpu.SMEM((batch,), jnp.int32),
            pltpu.VMEM((1, HEAD), F32),
            pltpu.VMEM((batch, width), BF16),
            pltpu.VMEM((4, width), F32),
            pltpu.VMEM((8, width), F32),
            pltpu.VMEM((LOCAL_BLOCKS, 4 * w_query.shape[2] // HEAD, k_local.shape[1] // LOCAL_BLOCKS), F32),
            pltpu.VMEM((n, 4, width), BF16),
            pltpu.VMEM((n, 4, width), BF16),
            pltpu.VMEM((8, ff), F32),
            pltpu.VMEM((8, ff), F32),
            pltpu.SemaphoreType.DMA((8 + 3 * QKV_CHUNKS + 2 * ROW_CHUNKS + COL_CHUNKS + K_PIECES,)),
            pltpu.SemaphoreType.DMA((2, n - 1)),
            pltpu.SemaphoreType.DMA((2, n - 1)),
            pltpu.SemaphoreType.DMA((COL_DOTS, n - 1)),
            pltpu.SemaphoreType.DMA((COL_DOTS, n - 1)),
        ],
        compiler_params=pltpu.CompilerParams(vmem_limit_bytes=LAYER0_MIB * MIB, collective_id=0, has_side_effects=True),
    )(*(in_hbm(value) for value in args))


def attn_kernel(layer, block, window, pos_hbm, freq_hbm, x_ref, new_ref, gain_hbm, wq_hbm, wk_hbm, wv_hbm, wo, kbuf, v_hbm, klbuf, vlbuf,
                o_ref, k_out, v_out, kl_out, vl_out, vbuf, wq, wk, wv, pos_ref, freq_ref, gain_ref, xbuf, ebuf, tiles,
                load_sem, t_sem, kout_sem, vout_sem, loc_sem):
    batch, length = v_hbm.shape[0], v_hbm.shape[1]
    heads = wq.shape[1] // HEAD
    blocks = length // block

    def piece(i):
        return pl.ds(pl.multiple_of(i * block, block), block)

    def v_load(i):
        return COPY(v_hbm.at[:, piece(i), :], vbuf.at[:, piece(i), :], load_sem.at[6 + i])

    def k_back(i):
        return COPY(kbuf.at[:, piece(i), :], k_out.at[:, piece(i), :], kout_sem.at[i])

    def v_back(i):
        return COPY(vbuf.at[:, piece(i), :], v_out.at[:, piece(i), :], vout_sem.at[i])

    loads = Loads(load_sem)
    gain_copy, pos_copy, freq_copy = loads.add(gain_hbm.at[layer], gain_ref), loads.add(pos_hbm, pos_ref), loads.add(freq_hbm, freq_ref)
    wk_copy, wq_copy, wv_copy = loads.add(wk_hbm.at[layer], wk), loads.add(wq_hbm.at[layer], wq), loads.add(wv_hbm.at[layer], wv)
    start_all([gain_copy, pos_copy, freq_copy, wk_copy, wq_copy, wv_copy])
    for i in range(blocks):
        v_load(i).start()
    loc_back = [COPY(klbuf, kl_out, loc_sem.at[0]), COPY(vlbuf, vl_out, loc_sem.at[1])]

    xbuf[...] = jnp.zeros_like(xbuf)
    gain_copy.wait()
    xbuf[0:batch, :] = x_ref[...].astype(F32)
    normed = norm_rows(xbuf[...], gain_ref[0:1, :])
    pos_copy.wait()
    freq_copy.wait()
    tables = rope_tables(pos_ref, freq_ref, batch)
    wk_copy.wait()
    key_new = rotate(matmul(normed, wk[...]), *tables).astype(BF16)
    wq_copy.wait()
    queries = matmul(normed, wq[...])
    stacked, lhs = stack_queries(queries, tables, heads, batch)
    wv_copy.wait()
    for i in range(blocks):
        k_back(i).start()
    start_all(loc_back)
    value_new = matmul(normed, wv[...]).astype(BF16)
    new_weights = capped_exp(jnp.sum(stacked * per_head(key_new, heads), axis=-1, keepdims=True))
    rows = 4 * heads
    tile_rows = lax.broadcasted_iota(jnp.int32, (16, HEAD), 0)

    def with_row(buf, new_rows, b, slot):
        base = pl.multiple_of((slot // 16) * 16, 16)
        tile = buf[b, pl.ds(base, 16), :].astype(F32)
        new_row = jnp.broadcast_to(new_rows[b:b + 1, :].astype(F32), (16, HEAD))
        return base, jnp.where(tile_rows == slot - base, new_row, tile).astype(BF16)

    col_ids = lax.broadcasted_iota(jnp.int32, (rows, block), 1)
    limits = row_values([pos_ref[b] for b in range(batch)], rows, block)

    def score_step(i, total):
        keys = jnp.concatenate([kbuf[b, piece(i), :] for b in range(batch)], axis=1)
        weights = capped_exp(score_rows(lhs, keys))
        col_pos = col_ids + i * block
        weights = jnp.where(col_pos < limits, weights, jnp.where(col_pos == limits, new_weights, 0.0))
        ebuf[i] = weights
        return total + jnp.sum(weights, axis=-1, keepdims=True)

    total = lax.fori_loop(0, blocks, score_step, jnp.zeros((rows, 1), F32))
    inv_total = 1.0 / total

    def value_step(i, acc):
        v_load(i).wait()
        for b in range(batch):
            @pl.when(pos_ref[b] // block == i)
            def _():
                base, tile = with_row(vbuf, value_new, b, pos_ref[b])
                vbuf[b, pl.ds(base, 16), :] = tile
        values = jnp.concatenate([vbuf[b, piece(i), :] for b in range(batch)], axis=1)
        out = acc + matmul((ebuf[i] * inv_total).astype(BF16), values)
        v_back(i).start()
        return out

    mixed = lax.fori_loop(0, blocks, value_step, jnp.zeros((rows, batch * HEAD), F32))
    merged = merge_heads(pick_rows(mixed, heads, batch), heads)
    for i in range(blocks):
        k_back(i).wait()
    wait_all(loc_back)
    tile_copies = []
    for which, (buf, out, new_rows) in enumerate(((kbuf, k_out, key_new), (klbuf, kl_out, new_ref[0]), (vlbuf, vl_out, new_ref[1]))):
        for b in range(batch):
            i = which * batch + b
            base, tiles[i] = with_row(buf, new_rows, b, pos_ref[b] % window if which else pos_ref[b])
            tile_copies.append(COPY(tiles.at[i], out.at[b, pl.ds(base, 16), :], t_sem.at[i]))
    o_ref[...] = matmul(merged, wo[...]).astype(BF16)
    start_all(tile_copies)
    for i in range(blocks):
        v_back(i).wait()
    wait_all(tile_copies)


def attn_call(layer, block, positions, freqs, hidden, new_rows, gains, w_query, w_key, w_value, w_out, k_pre, v_cache, k_local, v_local):
    batch, length, head = v_cache.shape
    width, q_cols = w_query.shape[1:]
    blocks = length // block
    vmem = pl.BlockSpec(memory_space=pltpu.VMEM)
    hbm = pl.BlockSpec(memory_space=pl.ANY)
    cache = jax.ShapeDtypeStruct(v_cache.shape, BF16)
    local = jax.ShapeDtypeStruct(k_local.shape, BF16)
    return pl.pallas_call(
        functools.partial(attn_kernel, layer, block, k_local.shape[1]),
        name=f"attn{layer}",
        out_shape=(pltpu.VMEM((4, width), BF16), cache, cache, local, local),
        in_specs=[hbm, hbm, vmem, vmem] + [hbm] * 4 + [vmem, vmem, hbm, vmem, vmem],
        out_specs=(vmem, hbm, hbm, hbm, hbm),
        scratch_shapes=[
            pltpu.VMEM(v_cache.shape, BF16),
            pltpu.VMEM((width, q_cols), BF16),
            pltpu.VMEM((width, head), BF16),
            pltpu.VMEM((width, head), BF16),
            pltpu.SMEM((batch,), jnp.int32),
            pltpu.VMEM((1, head), F32),
            pltpu.VMEM((4, width), F32),
            pltpu.VMEM((8, width), F32),
            pltpu.VMEM((blocks, 4 * q_cols // head, block), F32),
            pltpu.VMEM((3 * batch, 16, head), BF16),
            pltpu.SemaphoreType.DMA((6 + blocks,)),
            pltpu.SemaphoreType.DMA((3 * batch,)),
            pltpu.SemaphoreType.DMA((blocks,)),
            pltpu.SemaphoreType.DMA((blocks,)),
            pltpu.SemaphoreType.DMA((2,)),
        ],
        compiler_params=pltpu.CompilerParams(vmem_limit_bytes=ATTN_MIB * MIB),
    )(in_hbm(positions), in_hbm(freqs), in_vmem(hidden), in_vmem(new_rows), *(in_hbm(value) for value in (gains, w_query, w_key, w_value)),
      in_vmem(w_out), in_vmem(k_pre), in_hbm(v_cache), in_vmem(k_local), in_vmem(v_local))


def mlp_kernel(layer, n, o_ref, x_ref, gain_hbm, wg_hbm, wu_hbm, wd_hbm, x_out, wg, wu, wd, gain_ref, part1, part2, acc_g, acc_u,
               load_sem, send1, recv1, send2, recv2):
    me = lax.axis_index("tp")
    batch, width = x_ref.shape
    first_ex, second_ex = Exchange(n, me, part1, send1, recv1), Exchange(n, me, part2, send2, recv2)
    loads = Loads(load_sem)
    gain_copy = loads.add(gain_hbm.at[layer], gain_ref)
    gate, up = row_loads(loads, wg_hbm, layer, wg), row_loads(loads, wu_hbm, layer, wu)
    col_len = width // COL_CHUNKS
    down = [loads.add(wd_hbm.at[layer, :, pl.ds(i * col_len, col_len)], wd.at[:, pl.ds(i * col_len, col_len)]) for i in range(COL_CHUNKS)]
    down_dots = [(down[i:i + count], wd, 0, i * col_len, count * col_len) for i, count in ((0, 3), (3, 3), (6, 1), (7, 1))]
    part = ROW_CHUNKS // ROW_DOTS
    ordered = [gain_copy]
    for d in range(ROW_DOTS):
        ordered += gate[d * part:(d + 1) * part] + up[d * part:(d + 1) * part]
    start_all(ordered + down)
    met = greet(first_ex)
    part1[me] = o_ref[...]
    met()
    for h in range(2):
        first_ex.send(h * width // 2, (h + 1) * width // 2)
    gain_copy.wait()
    order = tuple((kind, d) for d in range(ROW_DOTS) for kind in range(2))
    x_out[...] = mlp_tail(first_ex.summed(batch), x_ref[...].astype(F32), gain_ref, gate, up, order, {}, down_dots, wg, wu, acc_g, acc_u, second_ex)
    first_ex.drain()
    second_ex.drain()


def mlp_call(layer, n, o_part, hidden, gains, w_gate, w_up, w_down):
    batch, width = hidden.shape
    ff = w_gate.shape[2]
    vmem = pl.BlockSpec(memory_space=pltpu.VMEM)
    hbm = pl.BlockSpec(memory_space=pl.ANY)
    return pl.pallas_call(
        functools.partial(mlp_kernel, layer, n),
        name=f"mlp{layer}",
        out_shape=jax.ShapeDtypeStruct((batch, width), BF16),
        in_specs=[vmem, vmem] + [hbm] * 4,
        out_specs=vmem,
        scratch_shapes=[
            pltpu.VMEM((width, ff), BF16),
            pltpu.VMEM((width, ff), BF16),
            pltpu.VMEM((ff, width), BF16),
            pltpu.VMEM((4, width), F32),
            pltpu.VMEM((n, 4, width), BF16),
            pltpu.VMEM((n, 4, width), BF16),
            pltpu.VMEM((8, ff), F32),
            pltpu.VMEM((8, ff), F32),
            pltpu.SemaphoreType.DMA((1 + 2 * ROW_CHUNKS + COL_CHUNKS,)),
            pltpu.SemaphoreType.DMA((2, n - 1)),
            pltpu.SemaphoreType.DMA((2, n - 1)),
            pltpu.SemaphoreType.DMA((COL_DOTS, n - 1)),
            pltpu.SemaphoreType.DMA((COL_DOTS, n - 1)),
        ],
        compiler_params=pltpu.CompilerParams(vmem_limit_bytes=44 * MIB + MIB // 2, collective_id=layer, has_side_effects=True),
    )(in_vmem(o_part), in_vmem(hidden), *(in_hbm(value) for value in (gains, w_gate, w_up, w_down)))


def decode_step(n, hidden, positions, k_local, v_local, k_global, v_global, w_query, w_key, w_value, w_out, w_gate, w_up, w_down, norm_scale):
    freqs = np.float32(ROPE_BASE) ** (np.float32(-2.0) * np.arange(HEAD // 2, dtype=np.float32) / np.float32(HEAD))
    freqs = jnp.asarray(np.concatenate([freqs, freqs])[None, :])
    k_loc, v_loc, k_glo, v_glo = (cache.reshape(cache.shape[0], cache.shape[1], HEAD) for cache in (k_local, v_local, k_global, v_global))
    heads = (norm_scale, w_query, w_key, w_value, w_out)
    hidden, new_rows, k_pre, k_loc, v_loc, w_next = layer0_call(n, positions, freqs, hidden, *heads, k_loc, v_loc, w_gate, w_up, w_down, k_glo)
    o_part, k_glo, v_glo, k_loc, v_loc = attn_call(1, 4096, positions, freqs, hidden, new_rows, *heads[:4], w_next, k_pre, v_glo, k_loc, v_loc)
    hidden = mlp_call(1, n, o_part, hidden, norm_scale, w_gate, w_up, w_down)
    return (hidden, k_loc.reshape(k_local.shape), v_loc.reshape(v_local.shape), k_glo.reshape(k_global.shape), v_glo.reshape(v_global.shape))


def solution(mesh):
    row_spec = P('dp', None)
    cache_spec = P('dp', None, 'tp', None)
    col_split = P(None, None, 'tp')
    row_split = P(None, 'tp', None)
    in_specs = (row_spec, P('dp'), cache_spec, cache_spec, cache_spec, cache_spec, col_split, col_split, col_split, row_split, col_split, col_split, row_split, P())
    out_specs = (row_spec, cache_spec, cache_spec, cache_spec, cache_spec)
    body = functools.partial(decode_step, mesh.shape['tp'])
    return jax.shard_map(body, mesh=mesh, in_specs=in_specs, out_specs=out_specs, check_vma=False)
```

```python
import functools

import jax
import jax.numpy as jnp
import numpy as np
from jax import lax
from jax.experimental import pallas as pl
from jax.experimental.pallas import tpu as pltpu
from jax.sharding import PartitionSpec as P

SOFT_CAP = 50.0
NORM_EPS = 1e-6
ROPE_BASE = 10000.0
HEAD = 128
MIB = 1024 * 1024
F32 = jnp.float32
BF16 = jnp.bfloat16
ROW_CHUNKS, ROW_DOTS = 2, 2
COL_CHUNKS, COL_DOTS = 8, 4
GROUPS = ((0, 3), (3, 3), (6, 1), (7, 1))
K_EARLY = 2
TAIL_GROUPS = ((0, 6), (6, 5), (11, 3), (14, 2))
K_PIECES = 6
LOCAL_BLOCKS = 2
LAYER0_MIB, ATTN_MIB = 32, 32
QKV_CHUNKS = 4
COPY = pltpu.make_async_copy


def in_vmem(value):
    return pltpu.with_memory_space_constraint(value, pltpu.VMEM)


def in_hbm(value):
    return pltpu.with_memory_space_constraint(value, pltpu.HBM)


def norm_rows(values, gain_row):
    inv_rms = lax.rsqrt(jnp.mean(values * values, axis=-1, keepdims=True) + NORM_EPS)
    return (values * inv_rms * (1.0 + gain_row)).astype(BF16)


def matmul(lhs, rhs):
    return jnp.dot(lhs, rhs, preferred_element_type=F32)


def capped_exp(logits):
    return jnp.exp(SOFT_CAP * jnp.tanh(logits * HEAD ** -0.5 / SOFT_CAP))


def rotate(head, cos_part, sin_part):
    return head * cos_part + pltpu.roll(head, HEAD // 2, 1) * sin_part


def rope_tables(pos_ref, freq_ref, batch):
    row_id = lax.broadcasted_iota(jnp.int32, (8, HEAD), 0)
    pos_rows = jnp.full((8, HEAD), pos_ref[0], jnp.int32)
    for b in range(1, batch):
        pos_rows = jnp.where(row_id == b, pos_ref[b], pos_rows)
    angles = pos_rows.astype(F32) * freq_ref[...]
    lane_id = lax.broadcasted_iota(jnp.int32, (8, HEAD), 1)
    sin_part = jnp.sin(angles)
    return jnp.cos(angles), jnp.where(lane_id < HEAD // 2, -sin_part, sin_part)


def row_of(rows):
    return lax.broadcasted_iota(jnp.int32, (rows, HEAD), 0) % 4


def stack_queries(queries, tables, heads, batch):
    stacked = jnp.concatenate([rotate(queries[:, h * HEAD:(h + 1) * HEAD], *tables)[0:4] for h in range(heads)], axis=0)
    of_row = row_of(4 * heads)
    lhs = jnp.concatenate([jnp.where(of_row == b, stacked, 0.0) for b in range(batch)], axis=1).astype(BF16)
    return stacked.astype(BF16).astype(F32), lhs


def per_head(new_rows, heads):
    return jnp.concatenate([new_rows[0:4]] * heads, axis=0).astype(F32)


def row_values(values, rows, cols):
    of_col = lax.broadcasted_iota(jnp.int32, (rows, cols), 0) % 4
    out = jnp.full((rows, cols), values[0], jnp.int32)
    for b in range(1, len(values)):
        out = jnp.where(of_col == b, values[b], out)
    return out


def pick_rows(mixed, heads, batch):
    of_row = row_of(4 * heads)
    picked = jnp.zeros((4 * heads, HEAD), F32)
    for b in range(batch):
        picked = jnp.where(of_row == b, mixed[:, b * HEAD:(b + 1) * HEAD], picked)
    return picked


def merge_heads(picked, heads):
    return jnp.concatenate([picked[4 * h:4 * h + 4, :] for h in range(heads)], axis=1).astype(BF16)


def score_rows(lhs, keys):
    return lax.dot_general(lhs, keys, (((1,), (1,)), ((), ())), preferred_element_type=F32)


class Loads:
    def __init__(self, sem):
        self.sem, self.count = sem, 0

    def add(self, src, dst):
        self.count += 1
        return COPY(src, dst, self.sem.at[self.count - 1])


def start_all(copies):
    for copy in copies:
        copy.start()


def wait_all(copies):
    for copy in copies:
        copy.wait()


class Exchange:
    def __init__(self, n, me, buf, send_sem, recv_sem):
        self.me, self.n, self.buf, self.send_sem, self.recv_sem = me, n, buf, send_sem, recv_sem
        self.peers = [lax.rem(me // 4 + far // 4, 2) * 4 + lax.rem(me // 2 + far // 2, 2) * 2 + lax.rem(me + far, 2) for far in (6, 7, 4, 5, 2, 3, 1)]
        self.sent = []

    def send(self, first, last):
        cols, i, group = pl.ds(first, last - first), len(self.sent), []
        for k, peer in enumerate(self.peers):
            group.append(pltpu.make_async_remote_copy(
                src_ref=self.buf.at[self.me, :, cols], dst_ref=self.buf.at[self.me, :, cols],
                send_sem=self.send_sem.at[i, k], recv_sem=self.recv_sem.at[i, k], device_id={"tp": peer}))
            group[k].start()
        self.sent.append((group, first, last))

    def summed(self, batch):
        parts = []
        for group, first, last in self.sent:
            for copy in group:
                copy.wait_recv()
            acc = self.buf[0, :, first:last].astype(F32)
            for j in range(1, self.n):
                acc = acc + self.buf[j, :, first:last].astype(F32)
            parts.append(acc)
        return jnp.concatenate(parts, axis=1)[0:batch]

    def drain(self):
        for group, _, _ in self.sent:
            for copy in group:
                copy.wait_send()


def row_loads(loads, hbm, layer, buf):
    step = buf.shape[0] // ROW_CHUNKS
    return [loads.add(hbm.at[layer, pl.ds(i * step, step), :], buf.at[pl.ds(i * step, step), :]) for i in range(ROW_CHUNKS)]


def mlp_tail(branch, hidden, gain_ref, gate, up, order, after, down_dots, wg, wu, acc_g, acc_u, exchange):
    batch, width = hidden.shape
    mid = (hidden + norm_rows(branch, gain_ref[1:2, :]).astype(F32)).astype(BF16).astype(F32)
    pre = norm_rows(mid, gain_ref[2:3, :])
    part = ROW_CHUNKS // ROW_DOTS
    row_len = width // ROW_DOTS
    for kind, d in order:
        loads, weights, acc = (gate, wg, acc_g) if kind == 0 else (up, wu, acc_u)
        wait_all(loads[d * part:(d + 1) * part])
        rows = slice(d * row_len, (d + 1) * row_len)
        product = matmul(pre[:, rows], weights[rows, :])
        acc[0:batch, :] = product if d == 0 else acc[0:batch, :] + product
        start_all(after.get((kind, d), []))
    act = (jax.nn.gelu(acc_g[0:batch, :], approximate=True) * acc_u[0:batch, :]).astype(BF16)
    first = 0
    for loads, buf, row, col, cols in down_dots:
        wait_all(loads)
        last = first + cols
        exchange.buf[exchange.me, 0:batch, first:last] = matmul(act, buf[row:row + act.shape[1], col:col + cols]).astype(BF16)
        exchange.send(first, last)
        first = last
    total = exchange.summed(batch)
    return (mid + norm_rows(total, gain_ref[3:4, :]).astype(F32)).astype(BF16)


def greet(exchange):
    barrier = pltpu.get_barrier_semaphore()
    for peer in exchange.peers:
        pl.semaphore_signal(barrier, inc=1, device_id={"tp": peer})
    return lambda: pl.semaphore_wait(barrier, exchange.n - 1)


def layer0_kernel(n, pos_hbm, freq_hbm, x_in, gain_hbm, wq_hbm, wk_hbm, wv_hbm, wo_hbm, k_hbm, v_hbm, wg_hbm, wu_hbm, wd_hbm, kg_hbm,
                  x_out, new_out, k_pre, kl_keep, vl_keep, wo_next, wg, wu, pos_ref, freq_ref, x_ref, gain_ref, xbuf, ebuf, part1, part2, acc_g, acc_u,
                  load_sem, send1, recv1, send2, recv2):
    me = lax.axis_index("tp")
    batch, width = x_in.shape
    window = k_hbm.shape[1]
    q_cols = wq_hbm.shape[2]
    heads = q_cols // HEAD
    half = width // 2
    first_ex, second_ex = Exchange(n, me, part1, send1, recv1), Exchange(n, me, part2, send2, recv2)
    loads = Loads(load_sem)
    small = [loads.add(x_in, x_ref), loads.add(gain_hbm.at[0], gain_ref), loads.add(pos_hbm, pos_ref), loads.add(freq_hbm, freq_ref)]
    wk_copy, wv_copy = loads.add(wk_hbm.at[0], wu.at[:, pl.ds(q_cols, HEAD)]), loads.add(wv_hbm.at[0], wu.at[:, pl.ds(q_cols + HEAD, HEAD)])
    step = width // QKV_CHUNKS
    qkv = [loads.add(wq_hbm.at[0, pl.ds(h * step, step), :], wu.at[pl.ds(h * step, step), pl.ds(0, q_cols)]) for h in range(QKV_CHUNKS)]
    k_copy, v_copy = loads.add(k_hbm, kl_keep), loads.add(v_hbm, vl_keep)
    wo_copy, wo_again = loads.add(wo_hbm.at[0], wo_next), loads.add(wo_hbm.at[1], wo_next)
    gate, up = row_loads(loads, wg_hbm, 0, wg), row_loads(loads, wu_hbm, 0, wu)
    ff, col_len = wg.shape[1], width // COL_CHUNKS
    places = [(buf, row, col * col_len) for buf, row in ((wg, 0), (wg, ff), (wu, 0)) for col in range(3)][0:COL_CHUNKS]
    down = [loads.add(wd_hbm.at[0, :, pl.ds(i * col_len, count * col_len)], places[i][0].at[pl.ds(places[i][1], ff), pl.ds(places[i][2], count * col_len)])
            for i, count in GROUPS]
    down_dots = [([load], *places[i], count * col_len) for load, (i, count) in zip(down, GROUPS)]
    k_len = kg_hbm.shape[1] // K_PIECES
    k_loads = [loads.add(kg_hbm.at[:, pl.ds(i * k_len, k_len), :], k_pre.at[:, pl.ds(i * k_len, k_len), :]) for i in range(K_PIECES)]
    start_all(small + [wk_copy, wv_copy] + qkv + [k_copy, v_copy, wo_copy] + gate)
    met = greet(first_ex)

    wait_all(small)
    xbuf[...] = jnp.zeros_like(xbuf)
    xbuf[0:batch, :] = x_ref[...].astype(F32)
    normed = norm_rows(xbuf[...], gain_ref[0:1, :])
    tables = rope_tables(pos_ref, freq_ref, batch)
    joint = jnp.zeros((8, q_cols + 2 * HEAD), F32)
    wait_all([wk_copy, wv_copy])
    for h in range(QKV_CHUNKS):
        qkv[h].wait()
        span = slice(h * step, (h + 1) * step)
        joint = joint + matmul(normed[:, span], wu[span, 0:q_cols + 2 * HEAD])
    start_all(up)
    key_new = rotate(joint[:, q_cols:q_cols + HEAD], *tables).astype(BF16)
    value_new = joint[:, q_cols + HEAD:q_cols + 2 * HEAD].astype(BF16)
    new_out[0] = key_new
    new_out[1] = value_new
    stacked, lhs = stack_queries(joint[:, 0:q_cols], tables, heads, batch)
    new_weights = capped_exp(jnp.sum(stacked * per_head(key_new, heads), axis=-1, keepdims=True))

    rows = 4 * heads
    block = window // LOCAL_BLOCKS
    slots = row_values([pos_ref[b] % window for b in range(batch)], rows, block)
    col_ids = lax.broadcasted_iota(jnp.int32, (rows, block), 1)

    def score_step(i, total):
        span = pl.ds(pl.multiple_of(i * block, block), block)
        keys = jnp.concatenate([kl_keep[b, span, :] for b in range(batch)], axis=1)
        weights = capped_exp(score_rows(lhs, keys))
        weights = jnp.where(col_ids + i * block == slots, 0.0, weights)
        ebuf[i] = weights
        return total + jnp.sum(weights, axis=-1, keepdims=True)

    def value_step(i, acc):
        span = pl.ds(pl.multiple_of(i * block, block), block)
        values = jnp.concatenate([vl_keep[b, span, :] for b in range(batch)], axis=1)
        return acc + matmul((ebuf[i] * inv_total).astype(BF16), values)

    k_copy.wait()
    inv_total = 1.0 / lax.fori_loop(0, LOCAL_BLOCKS, score_step, new_weights)
    v_copy.wait()
    mixed = lax.fori_loop(0, LOCAL_BLOCKS, value_step, jnp.zeros((rows, batch * HEAD), F32))
    new_probs = (new_weights * inv_total).astype(BF16).astype(F32)
    merged = merge_heads(pick_rows(mixed, heads, batch) + new_probs * per_head(value_new, heads), heads)

    met()
    wo_copy.wait()
    for h in range(2):
        part1[me, :, h * half:(h + 1) * half] = matmul(merged, wo_next[:, h * half:(h + 1) * half]).astype(BF16)
        first_ex.send(h * half, (h + 1) * half)
    start_all(k_loads[:K_EARLY])
    hidden = x_ref[...].astype(F32)
    order = ((0, 0), (0, 1), (1, 0), (1, 1))
    after = {(0, 1): down[:2], (1, 0): down[2:] + k_loads[K_EARLY:] + [wo_again]}
    x_out[...] = mlp_tail(first_ex.summed(batch), hidden, gain_ref, gate, up, order, after, down_dots, wg, wu, acc_g, acc_u, second_ex)
    first_ex.drain()
    second_ex.drain()
    wait_all(k_loads + [wo_again])


def layer0_call(n, positions, freqs, hidden, gains, w_query, w_key, w_value, w_out, k_local, v_local, w_gate, w_up, w_down, k_global):
    batch, width = hidden.shape
    ff = w_gate.shape[2]
    hbm = pl.BlockSpec(memory_space=pl.ANY)
    vmem = pl.BlockSpec(memory_space=pltpu.VMEM)
    args = (positions, freqs, hidden, gains, w_query, w_key, w_value, w_out, k_local, v_local, w_gate, w_up, w_down, k_global)
    return pl.pallas_call(
        functools.partial(layer0_kernel, n),
        name="layer0",
        out_shape=(pltpu.VMEM((batch, width), BF16), pltpu.VMEM((2, 8, HEAD), BF16), pltpu.VMEM(k_global.shape, BF16),
                   pltpu.VMEM(k_local.shape, BF16), pltpu.VMEM(v_local.shape, BF16), pltpu.VMEM(w_out.shape[1:], BF16)),
        in_specs=[hbm] * len(args),
        out_specs=(vmem,) * 6,
        scratch_shapes=[
            pltpu.VMEM((width, ff), BF16),
            pltpu.VMEM((width, ff), BF16),
            pltpu.SMEM((batch,), jnp.int32),
            pltpu.VMEM((1, HEAD), F32),
            pltpu.VMEM((batch, width), BF16),
            pltpu.VMEM((4, width), F32),
            pltpu.VMEM((8, width), F32),
            pltpu.VMEM((LOCAL_BLOCKS, 4 * w_query.shape[2] // HEAD, k_local.shape[1] // LOCAL_BLOCKS), F32),
            pltpu.VMEM((n, 4, width), BF16),
            pltpu.VMEM((n, 4, width), BF16),
            pltpu.VMEM((8, ff), F32),
            pltpu.VMEM((8, ff), F32),
            pltpu.SemaphoreType.DMA((8 + 3 * QKV_CHUNKS + 2 * ROW_CHUNKS + COL_CHUNKS + K_PIECES,)),
            pltpu.SemaphoreType.DMA((2, n - 1)),
            pltpu.SemaphoreType.DMA((2, n - 1)),
            pltpu.SemaphoreType.DMA((COL_DOTS, n - 1)),
            pltpu.SemaphoreType.DMA((COL_DOTS, n - 1)),
        ],
        compiler_params=pltpu.CompilerParams(vmem_limit_bytes=LAYER0_MIB * MIB, collective_id=0, has_side_effects=True),
    )(*(in_hbm(value) for value in args))


def attn_kernel(layer, block, window, pos_hbm, freq_hbm, x_ref, new_ref, gain_hbm, wq_hbm, wk_hbm, wv_hbm, wo, kbuf, v_hbm, klbuf, vlbuf,
                o_ref, k_out, v_out, kl_out, vl_out, vbuf, wq, wk, wv, pos_ref, freq_ref, gain_ref, xbuf, ebuf, tiles,
                load_sem, t_sem, kout_sem, vout_sem, loc_sem):
    batch, length = v_hbm.shape[0], v_hbm.shape[1]
    heads = wq.shape[1] // HEAD
    blocks = length // block

    def piece(i):
        return pl.ds(pl.multiple_of(i * block, block), block)

    def v_load(i):
        return COPY(v_hbm.at[:, piece(i), :], vbuf.at[:, piece(i), :], load_sem.at[6 + i])

    def k_back(i):
        return COPY(kbuf.at[:, piece(i), :], k_out.at[:, piece(i), :], kout_sem.at[i])

    def v_back(i):
        return COPY(vbuf.at[:, piece(i), :], v_out.at[:, piece(i), :], vout_sem.at[i])

    loads = Loads(load_sem)
    gain_copy, pos_copy, freq_copy = loads.add(gain_hbm.at[layer], gain_ref), loads.add(pos_hbm, pos_ref), loads.add(freq_hbm, freq_ref)
    wk_copy, wq_copy, wv_copy = loads.add(wk_hbm.at[layer], wk), loads.add(wq_hbm.at[layer], wq), loads.add(wv_hbm.at[layer], wv)
    start_all([gain_copy, pos_copy, freq_copy, wk_copy, wq_copy, wv_copy])
    for i in range(blocks):
        v_load(i).start()
    loc_back = [COPY(klbuf, kl_out, loc_sem.at[0]), COPY(vlbuf, vl_out, loc_sem.at[1])]

    xbuf[...] = jnp.zeros_like(xbuf)
    gain_copy.wait()
    xbuf[0:batch, :] = x_ref[...].astype(F32)
    normed = norm_rows(xbuf[...], gain_ref[0:1, :])
    pos_copy.wait()
    freq_copy.wait()
    tables = rope_tables(pos_ref, freq_ref, batch)
    wk_copy.wait()
    key_new = rotate(matmul(normed, wk[...]), *tables).astype(BF16)
    wq_copy.wait()
    queries = matmul(normed, wq[...])
    stacked, lhs = stack_queries(queries, tables, heads, batch)
    wv_copy.wait()
    value_new = matmul(normed, wv[...]).astype(BF16)
    new_weights = capped_exp(jnp.sum(stacked * per_head(key_new, heads), axis=-1, keepdims=True))
    rows = 4 * heads
    tile_rows = lax.broadcasted_iota(jnp.int32, (16, HEAD), 0)

    def with_row(buf, new_rows, b, slot):
        base = pl.multiple_of((slot // 16) * 16, 16)
        tile = buf[b, pl.ds(base, 16), :].astype(F32)
        new_row = jnp.broadcast_to(new_rows[b:b + 1, :].astype(F32), (16, HEAD))
        return base, jnp.where(tile_rows == slot - base, new_row, tile).astype(BF16)

    col_ids = lax.broadcasted_iota(jnp.int32, (rows, block), 1)
    limits = row_values([pos_ref[b] for b in range(batch)], rows, block)

    def score_step(i, total):
        @pl.when(i == 3)
        def _():
            for j in range(blocks):
                k_back(j).start()
            start_all(loc_back)

        keys = jnp.concatenate([kbuf[b, piece(i), :] for b in range(batch)], axis=1)
        weights = capped_exp(score_rows(lhs, keys))
        col_pos = col_ids + i * block
        weights = jnp.where(col_pos < limits, weights, jnp.where(col_pos == limits, new_weights, 0.0))
        ebuf[i] = weights
        return total + jnp.sum(weights, axis=-1, keepdims=True)

    total = lax.fori_loop(0, blocks, score_step, jnp.zeros((rows, 1), F32))
    inv_total = 1.0 / total

    def value_step(i, acc):
        v_load(i).wait()
        for b in range(batch):
            @pl.when(pos_ref[b] // block == i)
            def _():
                base, tile = with_row(vbuf, value_new, b, pos_ref[b])
                vbuf[b, pl.ds(base, 16), :] = tile
        values = jnp.concatenate([vbuf[b, piece(i), :] for b in range(batch)], axis=1)
        out = acc + matmul((ebuf[i] * inv_total).astype(BF16), values)
        v_back(i).start()
        return out

    mixed = lax.fori_loop(0, blocks, value_step, jnp.zeros((rows, batch * HEAD), F32))
    merged = merge_heads(pick_rows(mixed, heads, batch), heads)
    for i in range(blocks):
        k_back(i).wait()
    wait_all(loc_back)
    tile_copies = []
    for which, (buf, out, new_rows) in enumerate(((kbuf, k_out, key_new), (klbuf, kl_out, new_ref[0]), (vlbuf, vl_out, new_ref[1]))):
        for b in range(batch):
            i = which * batch + b
            base, tiles[i] = with_row(buf, new_rows, b, pos_ref[b] % window if which else pos_ref[b])
            tile_copies.append(COPY(tiles.at[i], out.at[b, pl.ds(base, 16), :], t_sem.at[i]))
    o_ref[...] = matmul(merged, wo[...]).astype(BF16)
    start_all(tile_copies)
    for i in range(blocks):
        v_back(i).wait()
    wait_all(tile_copies)


def attn_call(layer, block, positions, freqs, hidden, new_rows, gains, w_query, w_key, w_value, w_out, k_pre, v_cache, k_local, v_local):
    batch, length, head = v_cache.shape
    width, q_cols = w_query.shape[1:]
    blocks = length // block
    vmem = pl.BlockSpec(memory_space=pltpu.VMEM)
    hbm = pl.BlockSpec(memory_space=pl.ANY)
    cache = jax.ShapeDtypeStruct(v_cache.shape, BF16)
    local = jax.ShapeDtypeStruct(k_local.shape, BF16)
    return pl.pallas_call(
        functools.partial(attn_kernel, layer, block, k_local.shape[1]),
        name=f"attn{layer}",
        out_shape=(pltpu.VMEM((4, width), BF16), cache, cache, local, local),
        in_specs=[hbm, hbm, vmem, vmem] + [hbm] * 4 + [vmem, vmem, hbm, vmem, vmem],
        out_specs=(vmem, hbm, hbm, hbm, hbm),
        scratch_shapes=[
            pltpu.VMEM(v_cache.shape, BF16),
            pltpu.VMEM((width, q_cols), BF16),
            pltpu.VMEM((width, head), BF16),
            pltpu.VMEM((width, head), BF16),
            pltpu.SMEM((batch,), jnp.int32),
            pltpu.VMEM((1, head), F32),
            pltpu.VMEM((4, width), F32),
            pltpu.VMEM((8, width), F32),
            pltpu.VMEM((blocks, 4 * q_cols // head, block), F32),
            pltpu.VMEM((3 * batch, 16, head), BF16),
            pltpu.SemaphoreType.DMA((6 + blocks,)),
            pltpu.SemaphoreType.DMA((3 * batch,)),
            pltpu.SemaphoreType.DMA((blocks,)),
            pltpu.SemaphoreType.DMA((blocks,)),
            pltpu.SemaphoreType.DMA((2,)),
        ],
        compiler_params=pltpu.CompilerParams(vmem_limit_bytes=ATTN_MIB * MIB),
    )(in_hbm(positions), in_hbm(freqs), in_vmem(hidden), in_vmem(new_rows), *(in_hbm(value) for value in (gains, w_query, w_key, w_value)),
      in_vmem(w_out), in_vmem(k_pre), in_hbm(v_cache), in_vmem(k_local), in_vmem(v_local))


def mlp_kernel(layer, n, o_ref, x_ref, gain_hbm, wg_hbm, wu_hbm, wd_hbm, x_out, wg, wu, wd, gain_ref, part1, part2, acc_g, acc_u,
               load_sem, send1, recv1, send2, recv2):
    me = lax.axis_index("tp")
    batch, width = x_ref.shape
    first_ex, second_ex = Exchange(n, me, part1, send1, recv1), Exchange(n, me, part2, send2, recv2)
    loads = Loads(load_sem)
    gain_copy = loads.add(gain_hbm.at[layer], gain_ref)
    gate, up = row_loads(loads, wg_hbm, layer, wg), row_loads(loads, wu_hbm, layer, wu)
    col_len = width // 16
    down = [loads.add(wd_hbm.at[layer, :, pl.ds(i * col_len, count * col_len)], wd.at[:, pl.ds(i * col_len, count * col_len)]) for i, count in TAIL_GROUPS]
    down_dots = [([load], wd, 0, i * col_len, count * col_len) for load, (i, count) in zip(down, TAIL_GROUPS)]
    part = ROW_CHUNKS // ROW_DOTS
    ordered = [gain_copy]
    for d in range(ROW_DOTS):
        ordered += gate[d * part:(d + 1) * part] + up[d * part:(d + 1) * part]
    start_all(ordered + down)
    met = greet(first_ex)
    part1[me] = o_ref[...]
    met()
    for h in range(2):
        first_ex.send(h * width // 2, (h + 1) * width // 2)
    gain_copy.wait()
    order = tuple((kind, d) for d in range(ROW_DOTS) for kind in range(2))
    x_out[...] = mlp_tail(first_ex.summed(batch), x_ref[...].astype(F32), gain_ref, gate, up, order, {}, down_dots, wg, wu, acc_g, acc_u, second_ex)
    first_ex.drain()
    second_ex.drain()


def mlp_call(layer, n, o_part, hidden, gains, w_gate, w_up, w_down):
    batch, width = hidden.shape
    ff = w_gate.shape[2]
    vmem = pl.BlockSpec(memory_space=pltpu.VMEM)
    hbm = pl.BlockSpec(memory_space=pl.ANY)
    return pl.pallas_call(
        functools.partial(mlp_kernel, layer, n),
        name=f"mlp{layer}",
        out_shape=jax.ShapeDtypeStruct((batch, width), BF16),
        in_specs=[vmem, vmem] + [hbm] * 4,
        out_specs=vmem,
        scratch_shapes=[
            pltpu.VMEM((width, ff), BF16),
            pltpu.VMEM((width, ff), BF16),
            pltpu.VMEM((ff, width), BF16),
            pltpu.VMEM((4, width), F32),
            pltpu.VMEM((n, 4, width), BF16),
            pltpu.VMEM((n, 4, width), BF16),
            pltpu.VMEM((8, ff), F32),
            pltpu.VMEM((8, ff), F32),
            pltpu.SemaphoreType.DMA((1 + 2 * ROW_CHUNKS + COL_CHUNKS,)),
            pltpu.SemaphoreType.DMA((2, n - 1)),
            pltpu.SemaphoreType.DMA((2, n - 1)),
            pltpu.SemaphoreType.DMA((4, n - 1)),
            pltpu.SemaphoreType.DMA((4, n - 1)),
        ],
        compiler_params=pltpu.CompilerParams(vmem_limit_bytes=44 * MIB + MIB // 2, collective_id=layer, has_side_effects=True),
    )(in_vmem(o_part), in_vmem(hidden), *(in_hbm(value) for value in (gains, w_gate, w_up, w_down)))


def decode_step(n, hidden, positions, k_local, v_local, k_global, v_global, w_query, w_key, w_value, w_out, w_gate, w_up, w_down, norm_scale):
    freqs = np.float32(ROPE_BASE) ** (np.float32(-2.0) * np.arange(HEAD // 2, dtype=np.float32) / np.float32(HEAD))
    freqs = jnp.asarray(np.concatenate([freqs, freqs])[None, :])
    k_loc, v_loc, k_glo, v_glo = (cache.reshape(cache.shape[0], cache.shape[1], HEAD) for cache in (k_local, v_local, k_global, v_global))
    heads = (norm_scale, w_query, w_key, w_value, w_out)
    hidden, new_rows, k_pre, k_loc, v_loc, w_next = layer0_call(n, positions, freqs, hidden, *heads, k_loc, v_loc, w_gate, w_up, w_down, k_glo)
    o_part, k_glo, v_glo, k_loc, v_loc = attn_call(1, 4096, positions, freqs, hidden, new_rows, *heads[:4], w_next, k_pre, v_glo, k_loc, v_loc)
    hidden = mlp_call(1, n, o_part, hidden, norm_scale, w_gate, w_up, w_down)
    return (hidden, k_loc.reshape(k_local.shape), v_loc.reshape(v_local.shape), k_glo.reshape(k_global.shape), v_glo.reshape(v_global.shape))


def solution(mesh):
    row_spec = P('dp', None)
    cache_spec = P('dp', None, 'tp', None)
    col_split = P(None, None, 'tp')
    row_split = P(None, 'tp', None)
    in_specs = (row_spec, P('dp'), cache_spec, cache_spec, cache_spec, cache_spec, col_split, col_split, col_split, row_split, col_split, col_split, row_split, P())
    out_specs = (row_spec, cache_spec, cache_spec, cache_spec, cache_spec)
    body = functools.partial(decode_step, mesh.shape['tp'])
    return jax.shard_map(body, mesh=mesh, in_specs=in_specs, out_specs=out_specs, check_vma=False)
```

```python
import functools

import jax
import jax.numpy as jnp
import numpy as np
from jax import lax
from jax.experimental import pallas as pl
from jax.experimental.pallas import tpu as pltpu
from jax.sharding import PartitionSpec as P

SOFT_CAP = 50.0
NORM_EPS = 1e-6
ROPE_BASE = 10000.0
HEAD = 128
MIB = 1024 * 1024
F32 = jnp.float32
BF16 = jnp.bfloat16
ROW_CHUNKS, ROW_DOTS = 2, 2
COL_CHUNKS, COL_DOTS = 8, 4
GROUPS = ((0, 3), (3, 3), (6, 1), (7, 1))
K_EARLY = 2
TAIL_GROUPS = ((0, 6), (6, 5), (11, 3), (14, 2))
K_PIECES = 6
LOCAL_BLOCKS = 2
LAYER0_MIB, ATTN_MIB = 32, 32
QKV_CHUNKS = 4
COPY = pltpu.make_async_copy


def in_vmem(value):
    return pltpu.with_memory_space_constraint(value, pltpu.VMEM)


def in_hbm(value):
    return pltpu.with_memory_space_constraint(value, pltpu.HBM)


def norm_rows(values, gain_row):
    inv_rms = lax.rsqrt(jnp.mean(values * values, axis=-1, keepdims=True) + NORM_EPS)
    return (values * inv_rms * (1.0 + gain_row)).astype(BF16)


def matmul(lhs, rhs):
    return jnp.dot(lhs, rhs, preferred_element_type=F32)


def capped_exp(logits):
    return jnp.exp(SOFT_CAP * jnp.tanh(logits * HEAD ** -0.5 / SOFT_CAP))


def rotate(head, cos_part, sin_part):
    return head * cos_part + pltpu.roll(head, HEAD // 2, 1) * sin_part


def rope_tables(pos_ref, freq_ref, batch):
    row_id = lax.broadcasted_iota(jnp.int32, (8, HEAD), 0)
    pos_rows = jnp.full((8, HEAD), pos_ref[0], jnp.int32)
    for b in range(1, batch):
        pos_rows = jnp.where(row_id == b, pos_ref[b], pos_rows)
    angles = pos_rows.astype(F32) * freq_ref[...]
    lane_id = lax.broadcasted_iota(jnp.int32, (8, HEAD), 1)
    sin_part = jnp.sin(angles)
    return jnp.cos(angles), jnp.where(lane_id < HEAD // 2, -sin_part, sin_part)


def row_of(rows):
    return lax.broadcasted_iota(jnp.int32, (rows, HEAD), 0) % 4


def stack_queries(queries, tables, heads, batch):
    stacked = jnp.concatenate([rotate(queries[:, h * HEAD:(h + 1) * HEAD], *tables)[0:4] for h in range(heads)], axis=0)
    of_row = row_of(4 * heads)
    lhs = jnp.concatenate([jnp.where(of_row == b, stacked, 0.0) for b in range(batch)], axis=1).astype(BF16)
    return stacked.astype(BF16).astype(F32), lhs


def per_head(new_rows, heads):
    return jnp.concatenate([new_rows[0:4]] * heads, axis=0).astype(F32)


def row_values(values, rows, cols):
    of_col = lax.broadcasted_iota(jnp.int32, (rows, cols), 0) % 4
    out = jnp.full((rows, cols), values[0], jnp.int32)
    for b in range(1, len(values)):
        out = jnp.where(of_col == b, values[b], out)
    return out


def pick_rows(mixed, heads, batch):
    of_row = row_of(4 * heads)
    picked = jnp.zeros((4 * heads, HEAD), F32)
    for b in range(batch):
        picked = jnp.where(of_row == b, mixed[:, b * HEAD:(b + 1) * HEAD], picked)
    return picked


def merge_heads(picked, heads):
    return jnp.concatenate([picked[4 * h:4 * h + 4, :] for h in range(heads)], axis=1).astype(BF16)


def score_rows(lhs, keys):
    return lax.dot_general(lhs, keys, (((1,), (1,)), ((), ())), preferred_element_type=F32)


class Loads:
    def __init__(self, sem):
        self.sem, self.count = sem, 0

    def add(self, src, dst):
        self.count += 1
        return COPY(src, dst, self.sem.at[self.count - 1])


def start_all(copies):
    for copy in copies:
        copy.start()


def wait_all(copies):
    for copy in copies:
        copy.wait()


class Exchange:
    def __init__(self, n, me, buf, send_sem, recv_sem):
        self.me, self.n, self.buf, self.send_sem, self.recv_sem = me, n, buf, send_sem, recv_sem
        self.peers = [lax.rem(me // 4 + far // 4, 2) * 4 + lax.rem(me // 2 + far // 2, 2) * 2 + lax.rem(me + far, 2) for far in (6, 7, 4, 5, 2, 3, 1)]
        self.sent = []

    def send(self, first, last):
        cols, i, group = pl.ds(first, last - first), len(self.sent), []
        for k, peer in enumerate(self.peers):
            group.append(pltpu.make_async_remote_copy(
                src_ref=self.buf.at[self.me, :, cols], dst_ref=self.buf.at[self.me, :, cols],
                send_sem=self.send_sem.at[i, k], recv_sem=self.recv_sem.at[i, k], device_id={"tp": peer}))
            group[k].start()
        self.sent.append((group, first, last))

    def summed_norm(self, batch, gain_row):
        parts, squares, gain = [], [], 1.0 + gain_row
        for group, first, last in self.sent:
            for copy in group:
                copy.wait_recv()
            acc = self.buf[0, :, first:last].astype(F32)
            for j in range(1, self.n):
                acc = acc + self.buf[j, :, first:last].astype(F32)
            acc = acc[0:batch]
            parts.append(acc)
            squares.append(jnp.sum(acc * acc, axis=-1, keepdims=True))
        inv_rms = lax.rsqrt(sum(squares) / self.buf.shape[2] + NORM_EPS)
        return jnp.concatenate([(part * inv_rms * gain[:, first:last]).astype(BF16) for part, (_, first, last) in zip(parts, self.sent)], axis=1)

    def drain(self):
        for group, _, _ in self.sent:
            for copy in group:
                copy.wait_send()


def row_loads(loads, hbm, layer, buf):
    step = buf.shape[0] // ROW_CHUNKS
    return [loads.add(hbm.at[layer, pl.ds(i * step, step), :], buf.at[pl.ds(i * step, step), :]) for i in range(ROW_CHUNKS)]


def mlp_tail(branch, hidden, gain_ref, gate, up, order, after, down_dots, wg, wu, acc_g, acc_u, exchange):
    batch, width = hidden.shape
    mid = (hidden + branch.astype(F32)).astype(BF16).astype(F32)
    pre = norm_rows(mid, gain_ref[2:3, :])
    part = ROW_CHUNKS // ROW_DOTS
    row_len = width // ROW_DOTS
    for kind, d in order:
        loads, weights, acc = (gate, wg, acc_g) if kind == 0 else (up, wu, acc_u)
        wait_all(loads[d * part:(d + 1) * part])
        rows = slice(d * row_len, (d + 1) * row_len)
        product = matmul(pre[:, rows], weights[rows, :])
        acc[0:batch, :] = product if d == 0 else acc[0:batch, :] + product
        start_all(after.get((kind, d), []))
    act = (jax.nn.gelu(acc_g[0:batch, :], approximate=True) * acc_u[0:batch, :]).astype(BF16)
    first = 0
    for loads, buf, row, col, cols in down_dots:
        wait_all(loads)
        last = first + cols
        exchange.buf[exchange.me, 0:batch, first:last] = matmul(act, buf[row:row + act.shape[1], col:col + cols]).astype(BF16)
        exchange.send(first, last)
        first = last
    return (mid + exchange.summed_norm(batch, gain_ref[3:4, :]).astype(F32)).astype(BF16)


def greet(exchange):
    barrier = pltpu.get_barrier_semaphore()
    for peer in exchange.peers:
        pl.semaphore_signal(barrier, inc=1, device_id={"tp": peer})
    return lambda: pl.semaphore_wait(barrier, exchange.n - 1)


def layer0_kernel(n, pos_hbm, freq_hbm, x_in, gain_hbm, wq_hbm, wk_hbm, wv_hbm, wo_hbm, k_hbm, v_hbm, wg_hbm, wu_hbm, wd_hbm, kg_hbm,
                  x_out, new_out, k_pre, kl_keep, vl_keep, wo_next, wg, wu, pos_ref, freq_ref, x_ref, gain_ref, xbuf, ebuf, part1, part2, acc_g, acc_u,
                  load_sem, send1, recv1, send2, recv2):
    me = lax.axis_index("tp")
    batch, width = x_in.shape
    window = k_hbm.shape[1]
    q_cols = wq_hbm.shape[2]
    heads = q_cols // HEAD
    half = width // 2
    first_ex, second_ex = Exchange(n, me, part1, send1, recv1), Exchange(n, me, part2, send2, recv2)
    loads = Loads(load_sem)
    small = [loads.add(x_in, x_ref), loads.add(gain_hbm.at[0], gain_ref), loads.add(pos_hbm, pos_ref), loads.add(freq_hbm, freq_ref)]
    wk_copy, wv_copy = loads.add(wk_hbm.at[0], wu.at[:, pl.ds(q_cols, HEAD)]), loads.add(wv_hbm.at[0], wu.at[:, pl.ds(q_cols + HEAD, HEAD)])
    step = width // QKV_CHUNKS
    qkv = [loads.add(wq_hbm.at[0, pl.ds(h * step, step), :], wu.at[pl.ds(h * step, step), pl.ds(0, q_cols)]) for h in range(QKV_CHUNKS)]
    k_copy, v_copy = loads.add(k_hbm, kl_keep), loads.add(v_hbm, vl_keep)
    wo_copy, wo_again = loads.add(wo_hbm.at[0], wo_next), loads.add(wo_hbm.at[1], wo_next)
    gate, up = row_loads(loads, wg_hbm, 0, wg), row_loads(loads, wu_hbm, 0, wu)
    ff, col_len = wg.shape[1], width // COL_CHUNKS
    places = [(buf, row, col * col_len) for buf, row in ((wg, 0), (wg, ff), (wu, 0)) for col in range(3)][0:COL_CHUNKS]
    down = [loads.add(wd_hbm.at[0, :, pl.ds(i * col_len, count * col_len)], places[i][0].at[pl.ds(places[i][1], ff), pl.ds(places[i][2], count * col_len)])
            for i, count in GROUPS]
    down_dots = [([load], *places[i], count * col_len) for load, (i, count) in zip(down, GROUPS)]
    k_len = kg_hbm.shape[1] // K_PIECES
    k_loads = [loads.add(kg_hbm.at[:, pl.ds(i * k_len, k_len), :], k_pre.at[:, pl.ds(i * k_len, k_len), :]) for i in range(K_PIECES)]
    start_all(small + [wk_copy, wv_copy] + qkv + [k_copy, v_copy, wo_copy] + gate)
    met = greet(first_ex)

    wait_all(small)
    xbuf[...] = jnp.zeros_like(xbuf)
    xbuf[0:batch, :] = x_ref[...].astype(F32)
    normed = norm_rows(xbuf[...], gain_ref[0:1, :])
    tables = rope_tables(pos_ref, freq_ref, batch)
    joint = jnp.zeros((8, q_cols + 2 * HEAD), F32)
    wait_all([wk_copy, wv_copy])
    for h in range(QKV_CHUNKS):
        qkv[h].wait()
        span = slice(h * step, (h + 1) * step)
        joint = joint + matmul(normed[:, span], wu[span, 0:q_cols + 2 * HEAD])
    start_all(up)
    key_new = rotate(joint[:, q_cols:q_cols + HEAD], *tables).astype(BF16)
    value_new = joint[:, q_cols + HEAD:q_cols + 2 * HEAD].astype(BF16)
    new_out[0] = key_new
    new_out[1] = value_new
    stacked, lhs = stack_queries(joint[:, 0:q_cols], tables, heads, batch)
    new_weights = capped_exp(jnp.sum(stacked * per_head(key_new, heads), axis=-1, keepdims=True))

    rows = 4 * heads
    block = window // LOCAL_BLOCKS
    slots = row_values([pos_ref[b] % window for b in range(batch)], rows, block)
    col_ids = lax.broadcasted_iota(jnp.int32, (rows, block), 1)

    def score_step(i, total):
        span = pl.ds(pl.multiple_of(i * block, block), block)
        keys = jnp.concatenate([kl_keep[b, span, :] for b in range(batch)], axis=1)
        weights = capped_exp(score_rows(lhs, keys))
        weights = jnp.where(col_ids + i * block == slots, 0.0, weights)
        ebuf[i] = weights
        return total + jnp.sum(weights, axis=-1, keepdims=True)

    def value_step(i, acc):
        span = pl.ds(pl.multiple_of(i * block, block), block)
        values = jnp.concatenate([vl_keep[b, span, :] for b in range(batch)], axis=1)
        return acc + matmul((ebuf[i] * inv_total).astype(BF16), values)

    k_copy.wait()
    inv_total = 1.0 / lax.fori_loop(0, LOCAL_BLOCKS, score_step, new_weights)
    v_copy.wait()
    mixed = lax.fori_loop(0, LOCAL_BLOCKS, value_step, jnp.zeros((rows, batch * HEAD), F32))
    new_probs = (new_weights * inv_total).astype(BF16).astype(F32)
    merged = merge_heads(pick_rows(mixed, heads, batch) + new_probs * per_head(value_new, heads), heads)

    met()
    wo_copy.wait()
    for h in range(2):
        part1[me, :, h * half:(h + 1) * half] = matmul(merged, wo_next[:, h * half:(h + 1) * half]).astype(BF16)
        first_ex.send(h * half, (h + 1) * half)
    start_all(k_loads[:K_EARLY])
    hidden = x_ref[...].astype(F32)
    order = ((0, 0), (0, 1), (1, 0), (1, 1))
    after = {(0, 0): down[:1], (0, 1): down[1:2], (1, 0): down[2:] + k_loads[K_EARLY:] + [wo_again]}
    x_out[...] = mlp_tail(first_ex.summed_norm(batch, gain_ref[1:2, :]), hidden, gain_ref, gate, up, order, after, down_dots, wg, wu, acc_g, acc_u, second_ex)
    first_ex.drain()
    second_ex.drain()
    wait_all(k_loads + [wo_again])


def layer0_call(n, positions, freqs, hidden, gains, w_query, w_key, w_value, w_out, k_local, v_local, w_gate, w_up, w_down, k_global):
    batch, width = hidden.shape
    ff = w_gate.shape[2]
    hbm = pl.BlockSpec(memory_space=pl.ANY)
    vmem = pl.BlockSpec(memory_space=pltpu.VMEM)
    args = (positions, freqs, hidden, gains, w_query, w_key, w_value, w_out, k_local, v_local, w_gate, w_up, w_down, k_global)
    return pl.pallas_call(
        functools.partial(layer0_kernel, n),
        name="layer0",
        out_shape=(pltpu.VMEM((batch, width), BF16), pltpu.VMEM((2, 8, HEAD), BF16), pltpu.VMEM(k_global.shape, BF16),
                   pltpu.VMEM(k_local.shape, BF16), pltpu.VMEM(v_local.shape, BF16), pltpu.VMEM(w_out.shape[1:], BF16)),
        in_specs=[hbm] * len(args),
        out_specs=(vmem,) * 6,
        scratch_shapes=[
            pltpu.VMEM((width, ff), BF16),
            pltpu.VMEM((width, ff), BF16),
            pltpu.SMEM((batch,), jnp.int32),
            pltpu.VMEM((1, HEAD), F32),
            pltpu.VMEM((batch, width), BF16),
            pltpu.VMEM((4, width), F32),
            pltpu.VMEM((8, width), F32),
            pltpu.VMEM((LOCAL_BLOCKS, 4 * w_query.shape[2] // HEAD, k_local.shape[1] // LOCAL_BLOCKS), F32),
            pltpu.VMEM((n, 4, width), BF16),
            pltpu.VMEM((n, 4, width), BF16),
            pltpu.VMEM((8, ff), F32),
            pltpu.VMEM((8, ff), F32),
            pltpu.SemaphoreType.DMA((8 + 3 * QKV_CHUNKS + 2 * ROW_CHUNKS + COL_CHUNKS + K_PIECES,)),
            pltpu.SemaphoreType.DMA((2, n - 1)),
            pltpu.SemaphoreType.DMA((2, n - 1)),
            pltpu.SemaphoreType.DMA((COL_DOTS, n - 1)),
            pltpu.SemaphoreType.DMA((COL_DOTS, n - 1)),
        ],
        compiler_params=pltpu.CompilerParams(vmem_limit_bytes=LAYER0_MIB * MIB, collective_id=0, has_side_effects=True),
    )(*(in_hbm(value) for value in args))


def attn_kernel(layer, block, window, pos_hbm, freq_hbm, x_ref, new_ref, gain_hbm, wq_hbm, wk_hbm, wv_hbm, wo, kbuf, v_hbm, klbuf, vlbuf,
                o_ref, k_out, v_out, kl_out, vl_out, vbuf, wq, wk, wv, pos_ref, freq_ref, gain_ref, xbuf, ebuf, tiles,
                load_sem, t_sem, kout_sem, vout_sem, loc_sem):
    batch, length = v_hbm.shape[0], v_hbm.shape[1]
    heads = wq.shape[1] // HEAD
    blocks = length // block

    def piece(i):
        return pl.ds(pl.multiple_of(i * block, block), block)

    def v_load(i):
        return COPY(v_hbm.at[:, piece(i), :], vbuf.at[:, piece(i), :], load_sem.at[6 + i])

    def k_back(i):
        return COPY(kbuf.at[:, piece(i), :], k_out.at[:, piece(i), :], kout_sem.at[i])

    def v_back(i):
        return COPY(vbuf.at[:, piece(i), :], v_out.at[:, piece(i), :], vout_sem.at[i])

    loads = Loads(load_sem)
    gain_copy, pos_copy, freq_copy = loads.add(gain_hbm.at[layer], gain_ref), loads.add(pos_hbm, pos_ref), loads.add(freq_hbm, freq_ref)
    wk_copy, wq_copy, wv_copy = loads.add(wk_hbm.at[layer], wk), loads.add(wq_hbm.at[layer], wq), loads.add(wv_hbm.at[layer], wv)
    start_all([gain_copy, pos_copy, freq_copy, wk_copy, wq_copy, wv_copy])
    for i in range(blocks):
        v_load(i).start()
    loc_back = [COPY(klbuf, kl_out, loc_sem.at[0]), COPY(vlbuf, vl_out, loc_sem.at[1])]

    xbuf[...] = jnp.zeros_like(xbuf)
    gain_copy.wait()
    xbuf[0:batch, :] = x_ref[...].astype(F32)
    normed = norm_rows(xbuf[...], gain_ref[0:1, :])
    pos_copy.wait()
    freq_copy.wait()
    tables = rope_tables(pos_ref, freq_ref, batch)
    wk_copy.wait()
    key_new = rotate(matmul(normed, wk[...]), *tables).astype(BF16)
    wq_copy.wait()
    queries = matmul(normed, wq[...])
    stacked, lhs = stack_queries(queries, tables, heads, batch)
    wv_copy.wait()
    value_new = matmul(normed, wv[...]).astype(BF16)
    new_weights = capped_exp(jnp.sum(stacked * per_head(key_new, heads), axis=-1, keepdims=True))
    rows = 4 * heads
    tile_rows = lax.broadcasted_iota(jnp.int32, (16, HEAD), 0)

    def with_row(buf, new_rows, b, slot):
        base = pl.multiple_of((slot // 16) * 16, 16)
        tile = buf[b, pl.ds(base, 16), :].astype(F32)
        new_row = jnp.broadcast_to(new_rows[b:b + 1, :].astype(F32), (16, HEAD))
        return base, jnp.where(tile_rows == slot - base, new_row, tile).astype(BF16)

    col_ids = lax.broadcasted_iota(jnp.int32, (rows, block), 1)
    limits = row_values([pos_ref[b] for b in range(batch)], rows, block)

    def score_step(i, total):
        @pl.when(i == 3)
        def _():
            for j in range(blocks):
                k_back(j).start()
            start_all(loc_back)

        keys = jnp.concatenate([kbuf[b, piece(i), :] for b in range(batch)], axis=1)
        weights = capped_exp(score_rows(lhs, keys))
        col_pos = col_ids + i * block
        weights = jnp.where(col_pos < limits, weights, jnp.where(col_pos == limits, new_weights, 0.0))
        ebuf[i] = weights
        return total + jnp.sum(weights, axis=-1, keepdims=True)

    total = lax.fori_loop(0, blocks, score_step, jnp.zeros((rows, 1), F32))
    inv_total = 1.0 / total

    def value_step(i, acc):
        v_load(i).wait()
        for b in range(batch):
            @pl.when(pos_ref[b] // block == i)
            def _():
                base, tile = with_row(vbuf, value_new, b, pos_ref[b])
                vbuf[b, pl.ds(base, 16), :] = tile
        values = jnp.concatenate([vbuf[b, piece(i), :] for b in range(batch)], axis=1)
        out = acc + matmul((ebuf[i] * inv_total).astype(BF16), values)
        v_back(i).start()
        return out

    mixed = lax.fori_loop(0, blocks, value_step, jnp.zeros((rows, batch * HEAD), F32))
    merged = merge_heads(pick_rows(mixed, heads, batch), heads)
    for i in range(blocks):
        k_back(i).wait()
    wait_all(loc_back)
    tile_copies = []
    for which, (buf, out, new_rows) in enumerate(((kbuf, k_out, key_new), (klbuf, kl_out, new_ref[0]), (vlbuf, vl_out, new_ref[1]))):
        for b in range(batch):
            i = which * batch + b
            base, tiles[i] = with_row(buf, new_rows, b, pos_ref[b] % window if which else pos_ref[b])
            tile_copies.append(COPY(tiles.at[i], out.at[b, pl.ds(base, 16), :], t_sem.at[i]))
    o_ref[...] = matmul(merged, wo[...]).astype(BF16)
    start_all(tile_copies)
    for i in range(blocks):
        v_back(i).wait()
    wait_all(tile_copies)


def attn_call(layer, block, positions, freqs, hidden, new_rows, gains, w_query, w_key, w_value, w_out, k_pre, v_cache, k_local, v_local):
    batch, length, head = v_cache.shape
    width, q_cols = w_query.shape[1:]
    blocks = length // block
    vmem = pl.BlockSpec(memory_space=pltpu.VMEM)
    hbm = pl.BlockSpec(memory_space=pl.ANY)
    cache = jax.ShapeDtypeStruct(v_cache.shape, BF16)
    local = jax.ShapeDtypeStruct(k_local.shape, BF16)
    return pl.pallas_call(
        functools.partial(attn_kernel, layer, block, k_local.shape[1]),
        name=f"attn{layer}",
        out_shape=(pltpu.VMEM((4, width), BF16), cache, cache, local, local),
        in_specs=[hbm, hbm, vmem, vmem] + [hbm] * 4 + [vmem, vmem, hbm, vmem, vmem],
        out_specs=(vmem, hbm, hbm, hbm, hbm),
        scratch_shapes=[
            pltpu.VMEM(v_cache.shape, BF16),
            pltpu.VMEM((width, q_cols), BF16),
            pltpu.VMEM((width, head), BF16),
            pltpu.VMEM((width, head), BF16),
            pltpu.SMEM((batch,), jnp.int32),
            pltpu.VMEM((1, head), F32),
            pltpu.VMEM((4, width), F32),
            pltpu.VMEM((8, width), F32),
            pltpu.VMEM((blocks, 4 * q_cols // head, block), F32),
            pltpu.VMEM((3 * batch, 16, head), BF16),
            pltpu.SemaphoreType.DMA((6 + blocks,)),
            pltpu.SemaphoreType.DMA((3 * batch,)),
            pltpu.SemaphoreType.DMA((blocks,)),
            pltpu.SemaphoreType.DMA((blocks,)),
            pltpu.SemaphoreType.DMA((2,)),
        ],
        compiler_params=pltpu.CompilerParams(vmem_limit_bytes=ATTN_MIB * MIB),
    )(in_hbm(positions), in_hbm(freqs), in_vmem(hidden), in_vmem(new_rows), *(in_hbm(value) for value in (gains, w_query, w_key, w_value)),
      in_vmem(w_out), in_vmem(k_pre), in_hbm(v_cache), in_vmem(k_local), in_vmem(v_local))


def mlp_kernel(layer, n, o_ref, x_ref, gain_hbm, wg_hbm, wu_hbm, wd_hbm, x_out, wg, wu, wd, gain_ref, part1, part2, acc_g, acc_u,
               load_sem, send1, recv1, send2, recv2):
    me = lax.axis_index("tp")
    batch, width = x_ref.shape
    first_ex, second_ex = Exchange(n, me, part1, send1, recv1), Exchange(n, me, part2, send2, recv2)
    loads = Loads(load_sem)
    gain_copy = loads.add(gain_hbm.at[layer], gain_ref)
    gate, up = row_loads(loads, wg_hbm, layer, wg), row_loads(loads, wu_hbm, layer, wu)
    col_len = width // 16
    down = [loads.add(wd_hbm.at[layer, :, pl.ds(i * col_len, count * col_len)], wd.at[:, pl.ds(i * col_len, count * col_len)]) for i, count in TAIL_GROUPS]
    down_dots = [([load], wd, 0, i * col_len, count * col_len) for load, (i, count) in zip(down, TAIL_GROUPS)]
    part = ROW_CHUNKS // ROW_DOTS
    ordered = [gain_copy]
    for d in range(ROW_DOTS):
        ordered += gate[d * part:(d + 1) * part] + up[d * part:(d + 1) * part]
    start_all(ordered + down)
    met = greet(first_ex)
    part1[me] = o_ref[...]
    met()
    for h in range(2):
        first_ex.send(h * width // 2, (h + 1) * width // 2)
    gain_copy.wait()
    order = tuple((kind, d) for d in range(ROW_DOTS) for kind in range(2))
    x_out[...] = mlp_tail(first_ex.summed_norm(batch, gain_ref[1:2, :]), x_ref[...].astype(F32), gain_ref, gate, up, order, {}, down_dots, wg, wu, acc_g, acc_u, second_ex)
    first_ex.drain()
    second_ex.drain()


def mlp_call(layer, n, o_part, hidden, gains, w_gate, w_up, w_down):
    batch, width = hidden.shape
    ff = w_gate.shape[2]
    vmem = pl.BlockSpec(memory_space=pltpu.VMEM)
    hbm = pl.BlockSpec(memory_space=pl.ANY)
    return pl.pallas_call(
        functools.partial(mlp_kernel, layer, n),
        name=f"mlp{layer}",
        out_shape=jax.ShapeDtypeStruct((batch, width), BF16),
        in_specs=[vmem, vmem] + [hbm] * 4,
        out_specs=vmem,
        scratch_shapes=[
            pltpu.VMEM((width, ff), BF16),
            pltpu.VMEM((width, ff), BF16),
            pltpu.VMEM((ff, width), BF16),
            pltpu.VMEM((4, width), F32),
            pltpu.VMEM((n, 4, width), BF16),
            pltpu.VMEM((n, 4, width), BF16),
            pltpu.VMEM((8, ff), F32),
            pltpu.VMEM((8, ff), F32),
            pltpu.SemaphoreType.DMA((1 + 2 * ROW_CHUNKS + COL_CHUNKS,)),
            pltpu.SemaphoreType.DMA((2, n - 1)),
            pltpu.SemaphoreType.DMA((2, n - 1)),
            pltpu.SemaphoreType.DMA((4, n - 1)),
            pltpu.SemaphoreType.DMA((4, n - 1)),
        ],
        compiler_params=pltpu.CompilerParams(vmem_limit_bytes=44 * MIB + MIB // 2, collective_id=layer, has_side_effects=True),
    )(in_vmem(o_part), in_vmem(hidden), *(in_hbm(value) for value in (gains, w_gate, w_up, w_down)))


def decode_step(n, hidden, positions, k_local, v_local, k_global, v_global, w_query, w_key, w_value, w_out, w_gate, w_up, w_down, norm_scale):
    freqs = np.float32(ROPE_BASE) ** (np.float32(-2.0) * np.arange(HEAD // 2, dtype=np.float32) / np.float32(HEAD))
    freqs = jnp.asarray(np.concatenate([freqs, freqs])[None, :])
    k_loc, v_loc, k_glo, v_glo = (cache.reshape(cache.shape[0], cache.shape[1], HEAD) for cache in (k_local, v_local, k_global, v_global))
    heads = (norm_scale, w_query, w_key, w_value, w_out)
    hidden, new_rows, k_pre, k_loc, v_loc, w_next = layer0_call(n, positions, freqs, hidden, *heads, k_loc, v_loc, w_gate, w_up, w_down, k_glo)
    o_part, k_glo, v_glo, k_loc, v_loc = attn_call(1, 4096, positions, freqs, hidden, new_rows, *heads[:4], w_next, k_pre, v_glo, k_loc, v_loc)
    hidden = mlp_call(1, n, o_part, hidden, norm_scale, w_gate, w_up, w_down)
    return (hidden, k_loc.reshape(k_local.shape), v_loc.reshape(v_local.shape), k_glo.reshape(k_global.shape), v_glo.reshape(v_global.shape))


def solution(mesh):
    row_spec = P('dp', None)
    cache_spec = P('dp', None, 'tp', None)
    col_split = P(None, None, 'tp')
    row_split = P(None, 'tp', None)
    in_specs = (row_spec, P('dp'), cache_spec, cache_spec, cache_spec, cache_spec, col_split, col_split, col_split, row_split, col_split, col_split, row_split, P())
    out_specs = (row_spec, cache_spec, cache_spec, cache_spec, cache_spec)
    body = functools.partial(decode_step, mesh.shape['tp'])
    return jax.shard_map(body, mesh=mesh, in_specs=in_specs, out_specs=out_specs, check_vma=False)
```
